128 devices in a mesh: mesh: 32 (over y, x_lo, z), member: 4 (over x_hi, core).
Axes of the slice: x: 4 (x_hi: 2, x_lo: 2; x = x_hi * 2 + x_lo), y: 4, z: 4, core: 2. Of those that a mesh axis runs over, the one named last changes fastest.
Arguments:
- node_states: bfloat16 [8, 16384, 512], P('member', 'mesh'), may hold values from -60 to 60
- projection: bfloat16 [512, 1536], P('member'), may hold values from -12 to 12
- output_weight: bfloat16 [512, 512], P('member'), may hold values from -0.25 to 0.25
- up_weight: bfloat16 [512, 2048], P('member'), may hold values from -0.25 to 0.25
- down_weight: bfloat16 [2048, 512], P('member'), may hold values from -0.125 to 0.125
- attention_gain: float32 [512], replicated, may hold values from 0.5 to 2
- feedforward_gain: float32 [512], replicated, may hold values from 0.5 to 2
- tile_lists: int32 [128, 8], P('mesh'), may hold values from 0 to 127, as said below
- tile_counts: int32 [128], P('mesh'), may hold values from 4 to 8, as said below
Outputs:
- updated_states: bfloat16 [8, 16384, 512], P('member', 'mesh')
The draws below stay inside these ranges and needn't reach their ends.
Inputs may be any that keep to these rules, and one draw needn't show every extreme that they name: `tile_lists`: entry 0 of tile t's list is t. Every entry names a tile of the device that holds t, or one of the last 4 tiles of the device before it, or one of the first 4 tiles of the device after it along mesh (the first and last devices are neighbours). The first tile_counts[t] entries are distinct; later entries are ignored. `tile_counts`: every device holds a tile whose count is 8.
All inputs are finite; a program needn't handle non-finite values.
Results may differ from the reference program's by a relative error of at most 0.0056.
Values may be sent and summed in bfloat16 or wider, within the bound.
A program may use at most 128 MiB of HBM per device.

```python
import math
import jax
import jax.numpy as jnp
from jax import lax

D = 512
HEADS = 4
FF = 2048
TILE = 128
TILES_DEV = 4
RIM_T = 4
KT = 8
MEMBERS = 8
TILES = 128
NODES = 16384


def draw_node_states(key, part):
    sample = jax.random.normal(key, (MEMBERS, NODES, D), jnp.float32)
    return jnp.clip(sample, -60.0, 60.0).astype(jnp.bfloat16)


def draw_projection(key, part):
    sample = jnp.clip(jax.random.normal(key, (D, 3 * D), jnp.float32), -6.0, 6.0) * D ** (-0.5)
    return jnp.clip(sample, -12.0, 12.0).astype(jnp.bfloat16)


def tile_plan(key):
    sample = jax.random.fold_in(key, 7)
    devices = TILES // TILES_DEV
    window_tiles = TILES_DEV + 2 * RIM_T
    tile_ids = jnp.arange(TILES, dtype=jnp.int32)
    owner = tile_ids // TILES_DEV
    inner = tile_ids % TILES_DEV
    tile_keys = jax.random.split(sample, TILES)

    def pick(tile_key, own):
        shuffled = jax.random.permutation(tile_key, window_tiles - 1).astype(jnp.int32)
        shuffled = jnp.where(shuffled >= own, shuffled + 1, shuffled)
        return jnp.concatenate([own[None], shuffled[:KT - 1]])
    entries = jax.vmap(pick)(tile_keys, inner + RIM_T)
    owner_col = owner[:, None]
    leading = jnp.mod(owner_col - 1, devices) * TILES_DEV + TILES_DEV - RIM_T + entries
    middle = owner_col * TILES_DEV + entries - RIM_T
    trailing = jnp.mod(owner_col + 1, devices) * TILES_DEV + entries - RIM_T - TILES_DEV
    global_ids = jnp.where(entries < RIM_T, leading, jnp.where(entries < RIM_T + TILES_DEV, middle, trailing))
    counts = jax.random.randint(jax.random.fold_in(sample, 1), (TILES,), (KT + 1) // 2, KT + 1).astype(jnp.int32)
    counts = jnp.where(inner == 0, KT, counts).astype(jnp.int32)
    column = jnp.arange(KT, dtype=jnp.int32)
    global_ids = jnp.where(column[None, :] < counts[:, None], global_ids, tile_ids[:, None])
    return (global_ids.astype(jnp.int32), counts)


def draw_tile_lists(key, part):
    return tile_plan(key)[0]


def draw_tile_counts(key, part):
    return tile_plan(key)[1]


def steps_of(own_key, shape, cuts, low, largest):
    level, own = 1.0, jax.random.fold_in(own_key, 6)
    for axis_at, blocks in cuts:
        steps = jnp.exp(jax.random.uniform(jax.random.fold_in(own, axis_at), (blocks,), jnp.float32, low / len(cuts), largest / len(cuts)))
        level = level * jnp.repeat(steps, shape[axis_at] // blocks).reshape([-1 if axis == axis_at else 1 for axis in range(len(shape))])
    return level


def normal_values(rng, shape, scale, reach, pieces=(), kind=jnp.bfloat16):
    loudness = steps_of(rng, shape, pieces, -0.22, 0.18) if pieces else 1.0
    result = jax.random.normal(rng, shape, jnp.float32) * scale * loudness
    return jnp.minimum(jnp.maximum(result, -reach), reach).astype(kind)


def setup_inputs(seed: int = 0) -> dict:
    key_list = jax.random.split(jax.random.key(seed), 10)
    return {
        "node_states": draw_node_states(jax.random.fold_in(key_list[9], 71), 0),
        "projection": draw_projection(jax.random.fold_in(key_list[9], 71), 0),
        "output_weight": normal_values(key_list[2], (D, D), D ** -0.5, 0.25, ((0, 4),)),
        "up_weight": normal_values(key_list[3], (D, FF), D ** -0.5, 0.25, ((0, 4),)),
        "down_weight": normal_values(key_list[4], (FF, D), FF ** -0.5, 0.125, ((0, 4),)),
        "attention_gain": jnp.clip(jnp.exp(jax.random.uniform(key_list[5], (D,), jnp.float32, math.log(0.5), math.log(2.0))), 0.5, 2.0),
        "feedforward_gain": jnp.clip(jnp.exp(jax.random.uniform(key_list[6], (D,), jnp.float32, math.log(0.5), math.log(2.0))), 0.5, 2.0),
        "tile_lists": draw_tile_lists(jax.random.fold_in(key_list[9], 71), 0),
        "tile_counts": draw_tile_counts(jax.random.fold_in(key_list[9], 71), 0),
    }


def layer_norm(node_rows, gain):
    values = node_rows.astype(jnp.float32)
    center = values - lax.optimization_barrier(jnp.mean(values, axis=-1, keepdims=True))
    spread = lax.optimization_barrier(jnp.mean(center * center, axis=-1, keepdims=True))
    return (center * lax.rsqrt(spread + 1e-05) * gain).astype(jnp.bfloat16)

def attend(queries, window, tile_ids, counts):
    members, groups, tile_rows, model_width = queries.shape
    entries = tile_ids.shape[1]
    head_size = model_width // HEADS
    picked = jnp.take(window, tile_ids.reshape(-1), axis=1)
    picked = picked.reshape(members, groups, entries * tile_rows, 2 * model_width)
    key_part = picked[..., :model_width].reshape(members, groups, entries * tile_rows, HEADS, head_size).astype(jnp.float32)
    value_part = picked[..., model_width:].reshape(members, groups, entries * tile_rows, HEADS, head_size).astype(jnp.float32)
    query_part = queries.reshape(members, groups, tile_rows, HEADS, head_size).astype(jnp.float32)
    scores = jnp.einsum('mgqhe,mgkhe->mghqk', query_part, key_part) / math.sqrt(head_size)
    usable = (jnp.arange(entries * tile_rows) // tile_rows)[None, :] < counts[:, None]
    scores = jnp.where(usable[None, :, None, None, :], scores, -jnp.inf)
    highest = lax.optimization_barrier(jnp.max(scores, axis=-1, keepdims=True))
    weights = jnp.exp(scores - highest)
    summed = lax.optimization_barrier(jnp.sum(weights, axis=-1, keepdims=True))
    rounded = lax.optimization_barrier(weights.astype(jnp.bfloat16)).astype(jnp.float32)
    blended = jnp.einsum('mghqk,mgkhe->mghqe', rounded, value_part) / summed
    blended = jnp.transpose(blended, (0, 1, 3, 2, 4)).reshape(members, groups, tile_rows, model_width)
    return blended.astype(jnp.bfloat16)

def reference(node_states, projection, output_weight, up_weight, down_weight, attention_gain, feedforward_gain, tile_lists, tile_counts):
    members, node_count, model_width = node_states.shape
    normed = layer_norm(node_states, attention_gain)

    def project(node_rows):
        projected = jnp.dot(node_rows, projection, preferred_element_type=jnp.float32)
        return (projected[:, :model_width].astype(jnp.bfloat16), projected[:, model_width:].astype(jnp.bfloat16))
    queries, pairs = lax.map(project, normed)
    window = pairs.reshape(members, TILES, TILE, 2 * model_width)
    grouped = jnp.transpose(queries.reshape(members, TILES // 2, 2, TILE, model_width), (1, 0, 2, 3, 4))
    lists_grouped = tile_lists.reshape(TILES // 2, 2, KT)
    counts_grouped = tile_counts.reshape(TILES // 2, 2)

    def one_group(element):
        return attend(element[0], window, element[1], element[2])
    attended = lax.map(one_group, (grouped, lists_grouped, counts_grouped))
    attended = jnp.transpose(attended, (1, 0, 2, 3, 4)).reshape(members, node_count, model_width)

    def finish(element):
        states, blended = element
        middle = (states.astype(jnp.float32) + jnp.dot(blended, output_weight, preferred_element_type=jnp.float32)).astype(jnp.bfloat16)
        middle = lax.optimization_barrier(middle)
        normed_second = layer_norm(middle, feedforward_gain)
        hidden = jax.nn.gelu(jnp.dot(normed_second, up_weight, preferred_element_type=jnp.float32), approximate=True).astype(jnp.bfloat16)
        return (middle.astype(jnp.float32) + jnp.dot(hidden, down_weight, preferred_element_type=jnp.float32)).astype(jnp.bfloat16)
    return lax.map(finish, (node_states, attended))
```

```python
import functools
import math

import jax
import jax.numpy as jnp
from jax import lax
from jax.experimental import pallas as pl
from jax.experimental.pallas import tpu as pltpu
from jax.sharding import PartitionSpec as P

HEADS = 4
TILE = 128
RIM_T = 4
HIDDEN_LOW = -1e30
MESH = pl.DeviceIdType.MESH
F32 = jnp.float32
BF16 = jnp.bfloat16

SPLIT = ((0, 2), (1, 1), (2, 2), (3, 2))


def normed(values, gain):
    values = values.astype(F32)
    center = values - jnp.mean(values, axis=-1, keepdims=True)
    spread = jnp.mean(center * center, axis=-1, keepdims=True)
    return (center * lax.rsqrt(spread + 1e-05) * gain).astype(BF16)


def dot_nn(a, b):
    return jnp.dot(a, b, preferred_element_type=F32)


def dot_nt(a, b):
    return lax.dot_general(a, b, (((1,), (1,)), ((), ())), preferred_element_type=F32)


def dot_tn(a, b):
    return lax.dot_general(a, b, (((0,), (0,)), ((), ())), preferred_element_type=F32)


def layer_kernel(
    geometry,
    x_hbm, wp_hbm, wo_hbm, wu_hbm, wd_hbm, gain1, gain2, lists, counts,
    out_ref,
    own, halo, wp, wo, wu, wd, wq_t, wv_t, xn, hn, q_t, kc, v_t, acc, top, total, bias, scores, hid,
    loc_sem, halo_send, halo_recv, p_send, p_recv,
    x_send, x_recv, y_send, y_recv, dx_send, dx_recv, dy_send, dy_recv,
):
    n_mesh, n_z, n_x, n_member = geometry
    members, rows, width = x_hbm.shape
    tiles = rows // TILE
    head = width // HEADS
    i = lax.axis_index("mesh")
    m = lax.axis_index("member")
    nxt = (i + 1) % n_mesh
    prv = (i + n_mesh - 1) % n_mesh
    x_lo = (i // n_z) % n_x
    y = i // (n_z * n_x)
    half = y % 2
    plane = n_z * n_x
    cross = (i + n_z - 2 * n_z * x_lo, (m + 2) % n_member)
    mate = (i, m + 1 - 2 * (m % 2))
    y_to = ((i + n_mesh + plane * (2 * x_lo - 1)) % n_mesh, m)
    y_from = ((i + n_mesh - plane * (2 * x_lo - 1)) % n_mesh, m)
    far = (m + 2) % n_member
    mate_far = (mate[1] + 2) % n_member

    barrier = pltpu.get_barrier_semaphore()
    for peer in ((nxt, m), (prv, m), cross, mate, y_to, y_from):
        pl.semaphore_signal(barrier, inc=1, device_id=peer, device_id_type=MESH)

    sources = (wp_hbm, wo_hbm, wu_hbm, wd_hbm)
    fulls = (wp, wo, wu, wd)

    def shard(w, owner):
        r = sources[w].shape[0]
        return fulls[w].at[pl.ds(pl.multiple_of(owner * r, 16), r), :]

    def piece(w, n, k, owner, which):
        r = sources[w].shape[0]
        size = r // 2 // n
        start = owner * r + which * (r // 2) + k * size
        return fulls[w].at[pl.ds(pl.multiple_of(start, 16), size), :]

    load_x = pltpu.make_async_copy(x_hbm, own, loc_sem.at[4])
    load_x.start()
    loads = [pltpu.make_async_copy(sources[w], shard(w, m), loc_sem.at[w]) for w in range(4)]
    for load in loads:
        load.start()

    pieces = []
    for w, n in SPLIT:
        for k in range(n):
            pieces.append((w, n, k))

    def remote(src, dst, send, recv, peer):
        return pltpu.make_async_remote_copy(
            src_ref=src, dst_ref=dst, send_sem=send, recv_sem=recv, device_id=peer, device_id_type=MESH
        )

    def halo_copy(side, b, j):
        src = own.at[b, pl.ds(pl.multiple_of(j * TILE, TILE), TILE), :]
        dst = halo.at[b, side, pl.ds(pl.multiple_of(j * TILE, TILE), TILE), :]
        peer = (nxt, m) if side == 0 else (prv, m)
        return remote(src, dst, halo_send.at[side, b, j], halo_recv.at[side, b, j], peer)

    def mate_copy(w, owner):
        return remote(shard(w, owner), shard(w, owner), p_send.at[w], p_recv.at[w], mate)

    def x_copy(p, owner):
        ref = piece(*pieces[p], owner, half)
        return remote(ref, ref, x_send.at[p], x_recv.at[p], cross)

    def y_copy(p, which):
        ref = piece(*pieces[p], far, which)
        return remote(ref, ref, y_send.at[p], y_recv.at[p], y_to)

    def dx_copy(p, owner):
        ref = piece(*pieces[p], owner, half)
        return remote(ref, ref, dx_send.at[p], dx_recv.at[p], mate)

    def dy_copy(p, owner):
        ref = piece(*pieces[p], owner, 1 - half)
        return remote(ref, ref, dy_send.at[p], dy_recv.at[p], mate)

    def pass_x(p):
        x_copy(p, far).wait_recv()
        y_copy(p, half).start()
        dx_copy(p, far).start()

    def pass_y(p):
        y_copy(p, 1 - half).wait_recv()
        dy_copy(p, far).start()

    def arrive(w):
        mate_copy(w, mate[1]).wait_recv()
        for p, entry in enumerate(pieces):
            if entry[0] == w:
                dx_copy(p, mate_far).wait_recv()
                dy_copy(p, mate_far).wait_recv()

    first = i * tiles - RIM_T
    all_tiles = n_mesh * tiles
    entries = lists.shape[1]
    locals_ = [[(lists[t, e] - first + all_tiles) % all_tiles for e in range(entries)] for t in range(tiles)]
    for kt in range(tiles + 2 * RIM_T):
        for t in range(tiles):
            hit = jnp.int32(0)
            for e in range(entries):
                used = jnp.logical_and(locals_[t][e] == kt, e < counts[t])
                hit = jnp.where(used, jnp.int32(1), hit)
            level = jnp.where(hit > 0, F32(0), F32(HIDDEN_LOW))
            bias[pl.ds(kt, 1), t * TILE:(t + 1) * TILE] = jnp.full((1, TILE), level, F32)

    load_x.wait()
    for load in loads:
        load.wait()
    pl.semaphore_wait(barrier, 6)

    for b in range(members):
        for j in range(tiles):
            for side in range(2):
                halo_copy(side, b, j).start()
    for w in range(4):
        for p, entry in enumerate(pieces):
            if entry[0] == w:
                x_copy(p, m).start()
        mate_copy(w, m).start()

    def norm_own(k, _):
        b = k // tiles
        at = pl.ds(pl.multiple_of((k % tiles) * TILE, TILE), TILE)
        xn[b, at, :] = normed(own[b, at, :], gain1[...])
        return 0

    lax.fori_loop(0, members * tiles, norm_own, 0)

    pass_x(0)
    pass_x(1)
    pass_x(2)
    pass_y(0)
    pass_y(1)
    arrive(0)
    wq_t[...] = jnp.transpose(wp[:, :width])
    wv_t[...] = jnp.transpose(wp[:, 2 * width:])
    scale = F32(math.log2(math.e) / math.sqrt(head))

    def project(source, n):
        keys = dot_nn(source[...], wp[:, width:2 * width]).astype(BF16)
        for h in range(HEADS):
            kc[h, :n, :] = keys[:, h * head:(h + 1) * head]
        v_t[:, :n] = dot_nt(wv_t[...], source[...]).astype(BF16)

    def attend(marks, opening):
        n = len(marks) * TILE
        for h in range(HEADS):
            feats = slice(h * head, (h + 1) * head)
            scores[h, :n, :] = dot_nn(kc[h, :n, :], q_t[feats, :])
        for h in range(HEADS):
            feats = slice(h * head, (h + 1) * head)
            best = None if opening else top[h]
            for k, mark in enumerate(marks):
                high = jnp.max(scores[h, k * TILE:(k + 1) * TILE, :], axis=0, keepdims=True) + mark
                best = high if best is None else jnp.maximum(best, high)
            parts, added = [], None
            for k, mark in enumerate(marks):
                part = jnp.exp2(scores[h, k * TILE:(k + 1) * TILE, :] - (best - mark))
                summed = jnp.sum(part, axis=0, keepdims=True)
                added = summed if added is None else added + summed
                parts.append(part.astype(BF16))
            product = dot_nn(v_t[feats, :n], jnp.concatenate(parts, axis=0))
            if opening:
                acc[h] = product
                total[h] = added
            else:
                fade = jnp.exp2(top[h] - best)
                acc[h] = acc[h] * fade + product
                total[h] = total[h] * fade + added
            top[h] = best

    def one_member(b, _):
        q_t[...] = (dot_nt(wq_t[...], xn[b]) * scale).astype(BF16)
        project(xn.at[b], rows)
        attend([bias[RIM_T + t:RIM_T + t + 1, :] for t in range(tiles)], True)

        @pl.when(b == 0)
        def _():
            pass_x(3)
            pass_x(4)
            pass_y(2)

        def one_step(j, _):
            for side in range(2):
                halo_copy(side, b, j).wait_recv()
                at = pl.ds(pl.multiple_of(j * TILE, TILE), TILE)
                hn[side * TILE:(side + 1) * TILE, :] = normed(halo[b, side, at, :], gain1[...])
            project(hn, 2 * TILE)
            attend([bias[pl.ds(j, 1), :], bias[pl.ds(j + RIM_T + tiles, 1), :]], False)

            @pl.when(jnp.logical_and(b == 0, j == 0))
            def _():
                pass_y(3)
                pass_x(5)

            @pl.when(jnp.logical_and(b == 0, j == 1))
            def _():
                pass_y(4)

            @pl.when(jnp.logical_and(b == 0, j == 2))
            def _():
                pass_x(6)
                pass_y(5)

            @pl.when(jnp.logical_and(b == 0, j == 3))
            def _():
                pass_y(6)
                arrive(1)
                arrive(2)
                arrive(3)

            return 0

        lax.fori_loop(0, tiles, one_step, 0)

        for h in range(HEADS):
            v_t[h * head:(h + 1) * head, :] = (acc[h] / total[h]).astype(BF16)

        def finish(r, _):
            block = rows // 2
            at = pl.ds(pl.multiple_of(r * block, block), block)
            middle = (own[b, at, :].astype(F32) + dot_tn(v_t[:, at], wo[...])).astype(BF16)
            second = normed(middle, gain2[...])
            inner = wu.shape[1]
            step = inner // 4
            for f in range(4):
                u = dot_nn(second, wu[:, f * step:(f + 1) * step])
                slope = math.sqrt(2.0 / math.pi)
                bent = jnp.tanh(u * (slope + (slope * 0.044715) * (u * u)))
                hid[:, f * step:(f + 1) * step] = (0.5 * u * (1.0 + bent)).astype(BF16)
            out_ref[b, at, :] = (middle.astype(F32) + dot_nn(hid[...], wd[...])).astype(BF16)
            return 0

        lax.fori_loop(0, 2, finish, 0)
        return 0

    lax.fori_loop(0, members, one_member, 0)

    for b in range(members):
        for j in range(tiles):
            for side in range(2):
                halo_copy(side, b, j).wait_send()
    for w in range(4):
        mate_copy(w, m).wait_send()
    for p in range(len(pieces)):
        x_copy(p, m).wait_send()
        y_copy(p, half).wait_send()
        dx_copy(p, far).wait_send()
        dy_copy(p, far).wait_send()


def solution(mesh):
    n_mesh, n_member = mesh.shape["mesh"], mesh.shape["member"]
    geometry = (n_mesh, 4, 2, n_member)

    def on_device(states, projection, output_w, up_w, down_w, gain1, gain2, lists, counts):
        members, rows, width = states.shape
        inner = up_w.shape[1]
        tiles = rows // TILE
        n_pieces = sum(n for _, n in SPLIT)
        hbm = pl.BlockSpec(memory_space=pl.ANY)
        vmem = pl.BlockSpec(memory_space=pltpu.VMEM)
        smem = pl.BlockSpec(memory_space=pltpu.SMEM)
        dma = pltpu.SemaphoreType.DMA
        return pl.pallas_call(
            functools.partial(layer_kernel, geometry),
            name="layer",
            out_shape=jax.ShapeDtypeStruct(states.shape, BF16),
            in_specs=[hbm] * 5 + [vmem] * 2 + [smem] * 2,
            out_specs=vmem,
            scratch_shapes=[
                pltpu.VMEM((members, rows, width), BF16),
                pltpu.VMEM((members, 2, rows, width), BF16),
                pltpu.VMEM((width, 3 * width), BF16),
                pltpu.VMEM((width, width), BF16),
                pltpu.VMEM((width, inner), BF16),
                pltpu.VMEM((inner, width), BF16),
                pltpu.VMEM((width, width), BF16),
                pltpu.VMEM((width, width), BF16),
                pltpu.VMEM((members, rows, width), BF16),
                pltpu.VMEM((2 * TILE, width), BF16),
                pltpu.VMEM((width, rows), BF16),
                pltpu.VMEM((HEADS, rows, width // HEADS), BF16),
                pltpu.VMEM((width, rows), BF16),
                pltpu.VMEM((HEADS, width // HEADS, rows), F32),
                pltpu.VMEM((HEADS, 1, rows), F32),
                pltpu.VMEM((HEADS, 1, rows), F32),
                pltpu.VMEM((tiles + 2 * RIM_T, rows), F32),
                pltpu.VMEM((HEADS, rows, rows), F32),
                pltpu.VMEM((rows // 2, inner), BF16),
                dma((5,)),
                dma((2, members, tiles)), dma((2, members, tiles)),
                dma((4,)), dma((4,)),
            ] + [dma((n_pieces,)) for _ in range(8)],
            compiler_params=pltpu.CompilerParams(
                collective_id=0, has_side_effects=True, vmem_limit_bytes=60 * 1024 * 1024
            ),
        )(
            states, projection, output_w, up_w, down_w,
            gain1.reshape(1, width), gain2.reshape(1, width), lists, counts,
        )

    in_specs = (
        P("member", "mesh", None),
        P("member", None),
        P("member", None),
        P("member", None),
        P("member", None),
        P(),
        P(),
        P("mesh", None),
        P("mesh"),
    )
    return jax.shard_map(
        on_device, mesh=mesh, in_specs=in_specs, out_specs=P("member", "mesh", None), check_vma=False
    )
```

```python
import functools
import math

import jax
import jax.numpy as jnp
from jax import lax
from jax.experimental import pallas as pl
from jax.experimental.pallas import tpu as pltpu
from jax.sharding import PartitionSpec as P

HEADS = 4
TILE = 128
RIM_T = 4
HIDDEN_LOW = -1e30
MESH = pl.DeviceIdType.MESH
F32 = jnp.float32
BF16 = jnp.bfloat16

SPLIT = ((0, 2), (1, 1), (2, 2), (3, 2))


def normed(values, gain):
    values = values.astype(F32)
    center = values - jnp.mean(values, axis=-1, keepdims=True)
    spread = jnp.mean(center * center, axis=-1, keepdims=True)
    return (center * lax.rsqrt(spread + 1e-05) * gain).astype(BF16)


def dot_nn(a, b):
    return jnp.dot(a, b, preferred_element_type=F32)


def dot_nt(a, b):
    return lax.dot_general(a, b, (((1,), (1,)), ((), ())), preferred_element_type=F32)


def dot_tn(a, b):
    return lax.dot_general(a, b, (((0,), (0,)), ((), ())), preferred_element_type=F32)


def layer_kernel(
    geometry,
    x_hbm, wp_hbm, wo_hbm, wu_hbm, wd_hbm, gain1_hbm, gain2_hbm, lists_hbm, counts_hbm,
    out_ref,
    own, halo, wp, wo, wu, wd, wq_t, wv_t, xn, hn, q_t, kc, v_t, acc, top, total, bias, scores, hid,
    gain1, gain2, lists, counts,
    loc_sem, halo_send, halo_recv, p_send, p_recv,
    x_send, x_recv, y_send, y_recv, dx_send, dx_recv, dy_send, dy_recv,
):
    n_mesh, n_z, n_x, n_member = geometry
    members, rows, width = x_hbm.shape
    tiles = rows // TILE
    head = width // HEADS
    i = lax.axis_index("mesh")
    m = lax.axis_index("member")
    nxt = (i + 1) % n_mesh
    prv = (i + n_mesh - 1) % n_mesh
    x_lo = (i // n_z) % n_x
    y = i // (n_z * n_x)
    half = y % 2
    plane = n_z * n_x
    cross = (i + n_z - 2 * n_z * x_lo, (m + 2) % n_member)
    mate = (i, m + 1 - 2 * (m % 2))
    y_to = ((i + n_mesh + plane * (2 * x_lo - 1)) % n_mesh, m)
    y_from = ((i + n_mesh - plane * (2 * x_lo - 1)) % n_mesh, m)
    far = (m + 2) % n_member
    mate_far = (mate[1] + 2) % n_member

    barrier = pltpu.get_barrier_semaphore()
    for peer in ((nxt, m), (prv, m), cross, mate, y_to, y_from):
        pl.semaphore_signal(barrier, inc=1, device_id=peer, device_id_type=MESH)

    sources = (wp_hbm, wo_hbm, wu_hbm, wd_hbm)
    fulls = (wp, wo, wu, wd)

    def shard(w, owner):
        r = sources[w].shape[0]
        return fulls[w].at[pl.ds(pl.multiple_of(owner * r, 16), r), :]

    def piece(w, n, k, owner, which):
        r = sources[w].shape[0]
        size = r // 2 // n
        start = owner * r + which * (r // 2) + k * size
        return fulls[w].at[pl.ds(pl.multiple_of(start, 16), size), :]

    smalls = [
        pltpu.make_async_copy(src, dst, loc_sem.at[5 + k])
        for k, (src, dst) in enumerate(
            ((lists_hbm, lists), (counts_hbm, counts), (gain1_hbm, gain1), (gain2_hbm, gain2))
        )
    ]
    for small in smalls:
        small.start()
    load_x = pltpu.make_async_copy(x_hbm, own, loc_sem.at[4])
    load_x.start()
    loads = [pltpu.make_async_copy(sources[w], shard(w, m), loc_sem.at[w]) for w in range(4)]
    for load in loads:
        load.start()

    pieces = []
    for w, n in SPLIT:
        for k in range(n):
            pieces.append((w, n, k))

    def remote(src, dst, send, recv, peer):
        return pltpu.make_async_remote_copy(
            src_ref=src, dst_ref=dst, send_sem=send, recv_sem=recv, device_id=peer, device_id_type=MESH
        )

    def halo_copy(side, b, j):
        src = own.at[b, pl.ds(pl.multiple_of(j * TILE, TILE), TILE), :]
        dst = halo.at[b, side, pl.ds(pl.multiple_of(j * TILE, TILE), TILE), :]
        peer = (nxt, m) if side == 0 else (prv, m)
        return remote(src, dst, halo_send.at[side, b, j], halo_recv.at[side, b, j], peer)

    def mate_copy(w, owner):
        return remote(shard(w, owner), shard(w, owner), p_send.at[w], p_recv.at[w], mate)

    def x_copy(p, owner):
        ref = piece(*pieces[p], owner, half)
        return remote(ref, ref, x_send.at[p], x_recv.at[p], cross)

    def y_copy(p, which):
        ref = piece(*pieces[p], far, which)
        return remote(ref, ref, y_send.at[p], y_recv.at[p], y_to)

    def dx_copy(p, owner):
        ref = piece(*pieces[p], owner, half)
        return remote(ref, ref, dx_send.at[p], dx_recv.at[p], mate)

    def dy_copy(p, owner):
        ref = piece(*pieces[p], owner, 1 - half)
        return remote(ref, ref, dy_send.at[p], dy_recv.at[p], mate)

    def pass_x(p):
        x_copy(p, far).wait_recv()
        y_copy(p, half).start()
        dx_copy(p, far).start()

    def pass_y(p):
        y_copy(p, 1 - half).wait_recv()
        dy_copy(p, far).start()

    def arrive(w):
        mate_copy(w, mate[1]).wait_recv()
        for p, entry in enumerate(pieces):
            if entry[0] == w:
                dx_copy(p, mate_far).wait_recv()
                dy_copy(p, mate_far).wait_recv()

    for small in smalls:
        small.wait()
    first = i * tiles - RIM_T
    all_tiles = n_mesh * tiles
    entries = lists.shape[1]
    locals_ = [[(lists[t, e] - first + all_tiles) % all_tiles for e in range(entries)] for t in range(tiles)]
    for kt in range(tiles + 2 * RIM_T):
        for t in range(tiles):
            hit = jnp.int32(0)
            for e in range(entries):
                used = jnp.logical_and(locals_[t][e] == kt, e < counts[t])
                hit = jnp.where(used, jnp.int32(1), hit)
            level = jnp.where(hit > 0, F32(0), F32(HIDDEN_LOW))
            bias[pl.ds(kt, 1), t * TILE:(t + 1) * TILE] = jnp.full((1, TILE), level, F32)

    with jax.named_scope("enter"):
        load_x.wait()
        for load in loads:
            load.wait()
        pl.semaphore_wait(barrier, 6)

    for b in range(members):
        for j in range(tiles):
            for side in range(2):
                halo_copy(side, b, j).start()
    for w in range(4):
        for p, entry in enumerate(pieces):
            if entry[0] == w:
                x_copy(p, m).start()
        mate_copy(w, m).start()

    def norm_own(k, _):
        b = k // tiles
        at = pl.ds(pl.multiple_of((k % tiles) * TILE, TILE), TILE)
        xn[b, at, :] = normed(own[b, at, :], gain1[...])
        return 0

    with jax.named_scope("norm_own"):
        lax.fori_loop(0, members * tiles, norm_own, 0)

    steps = members * tiles

    def halo_norm(s, slot):
        b, j = s // tiles, s % tiles
        at = pl.ds(pl.multiple_of(j * TILE, TILE), TILE)
        for side in range(2):
            hn[slot, side * TILE:(side + 1) * TILE, :] = normed(halo[b, side, at, :], gain1[...])

    def halo_wait(s):
        for side in range(2):
            halo_copy(side, s // tiles, s % tiles).wait_recv()

    with jax.named_scope("gather"):
        pass_x(0)
        pass_x(1)
        halo_wait(0)
        halo_norm(0, 0)
        pass_x(2)
        pass_y(0)
        pass_y(1)
        pass_x(3)
        arrive(0)
    with jax.named_scope("flip"):
        wq_t[...] = jnp.transpose(wp[:, :width])
        wv_t[...] = jnp.transpose(wp[:, 2 * width:])
    scale = F32(math.log2(math.e) / math.sqrt(head))

    def project(source, slot, n):
        keys = dot_nn(source[...], wp[:, width:2 * width]).astype(BF16)
        for h in range(HEADS):
            kc[slot, h, :n, :] = keys[:, h * head:(h + 1) * head]
        v_t[slot, :, :n] = dot_nt(wv_t[...], source[...]).astype(BF16)

    def attend(b, slot, marks, opening):
        n = len(marks) * TILE
        for h in range(HEADS):
            feats = slice(h * head, (h + 1) * head)
            scores[h, :n, :] = dot_nn(kc[slot, h, :n, :], q_t[b, feats, :])
        for h in range(HEADS):
            feats = slice(h * head, (h + 1) * head)
            best = None if opening else top[b, h]
            for k, mark in enumerate(marks):
                high = jnp.max(scores[h, k * TILE:(k + 1) * TILE, :], axis=0, keepdims=True) + mark
                best = high if best is None else jnp.maximum(best, high)
            parts, added = [], None
            for k, mark in enumerate(marks):
                part = jnp.exp2(scores[h, k * TILE:(k + 1) * TILE, :] - (best - mark))
                summed = jnp.sum(part, axis=0, keepdims=True)
                added = summed if added is None else added + summed
                parts.append(part.astype(BF16))
            product = dot_nn(v_t[slot, feats, :n], jnp.concatenate(parts, axis=0))
            if opening:
                acc[b, h] = product
                total[b, h] = added
            else:
                fade = jnp.exp2(top[b, h] - best)
                acc[b, h] = acc[b, h] * fade + product
                total[b, h] = total[b, h] * fade + added
            top[b, h] = best

    def own_project(b):
        q_t[b] = (dot_nt(wq_t[...], xn[b]) * scale).astype(BF16)
        project(xn.at[b], b, rows)

    def own_attend(b):
        attend(b, b, [bias[RIM_T + t:RIM_T + t + 1, :] for t in range(tiles)], True)

    def halo_project(slot):
        project(hn.at[slot], slot, 2 * TILE)

    def halo_attend(s, slot):
        b, j = s // tiles, s % tiles
        attend(b, slot, [bias[pl.ds(j, 1), :], bias[pl.ds(j + RIM_T + tiles, 1), :]], False)

    with jax.named_scope("own0"):
        own_project(0)
    with jax.named_scope("own1"):
        own_attend(0)
        own_project(1)
    pass_x(4)
    pass_y(2)
    with jax.named_scope("wait1"):
        halo_wait(1)
    with jax.named_scope("own2"):
        own_attend(1)
        halo_project(0)
        halo_norm(1, 1)

    def two_steps(t, _):
        s = 2 * t
        with jax.named_scope("wait2"):
            halo_wait(s + 2)

            @pl.when(t == 0)
            def _():
                pass_y(3)
                pass_x(5)

            @pl.when(t == 1)
            def _():
                pass_y(4)
                pass_y(5)

        with jax.named_scope("stepa"):
            halo_attend(s, 0)
            halo_project(1)
            halo_norm(s + 2, 0)
        with jax.named_scope("wait3"):
            halo_wait(s + 3)

            @pl.when(t == 0)
            def _():
                pass_x(6)

            @pl.when(t == 2)
            def _():
                pass_y(6)

        with jax.named_scope("stepb"):
            halo_attend(s + 1, 1)
            halo_project(0)
            halo_norm(s + 3, 1)
        return 0

    lax.fori_loop(0, steps // 2 - 1, two_steps, 0)
    with jax.named_scope("last"):
        halo_attend(steps - 2, 0)
        halo_project(1)
        halo_attend(steps - 1, 1)
    with jax.named_scope("gather2"):
        arrive(1)
        arrive(2)
        arrive(3)

    block = rows // 2
    inner = wu.shape[1]
    step = inner // 4
    slope = math.sqrt(2.0 / math.pi)

    def finish(b, _):
        with jax.named_scope("finish"):
            for h in range(HEADS):
                v_t[0, h * head:(h + 1) * head, :] = (acc[b, h] / total[b, h]).astype(BF16)
            for r in range(2):
                at = slice(r * block, (r + 1) * block)
                middle = (own[b, at, :].astype(F32) + dot_tn(v_t[0, :, at], wo[...])).astype(BF16)
                second = normed(middle, gain2[...])
                for f in range(4):
                    u = dot_nn(second, wu[:, f * step:(f + 1) * step])
                    bent = jnp.tanh(u * (slope + (slope * 0.044715) * (u * u)))
                    hid[r, :, f * step:(f + 1) * step] = (0.5 * u * (1.0 + bent)).astype(BF16)
                out_ref[b, at, :] = (middle.astype(F32) + dot_nn(hid[r], wd[...])).astype(BF16)
        return 0

    lax.fori_loop(0, members, finish, 0)

    for b in range(members):
        for j in range(tiles):
            for side in range(2):
                halo_copy(side, b, j).wait_send()
    for w in range(4):
        mate_copy(w, m).wait_send()
    for p in range(len(pieces)):
        x_copy(p, m).wait_send()
        y_copy(p, half).wait_send()
        dx_copy(p, far).wait_send()
        dy_copy(p, far).wait_send()


def solution(mesh):
    n_mesh, n_member = mesh.shape["mesh"], mesh.shape["member"]
    geometry = (n_mesh, 4, 2, n_member)

    def on_device(states, projection, output_w, up_w, down_w, gain1, gain2, lists, counts):
        members, rows, width = states.shape
        inner = up_w.shape[1]
        tiles = rows // TILE
        n_pieces = sum(n for _, n in SPLIT)
        hbm = pl.BlockSpec(memory_space=pl.ANY)
        vmem = pl.BlockSpec(memory_space=pltpu.VMEM)
        dma = pltpu.SemaphoreType.DMA
        return pl.pallas_call(
            functools.partial(layer_kernel, geometry),
            name="layer",
            out_shape=jax.ShapeDtypeStruct(states.shape, BF16),
            in_specs=[hbm] * 9,
            out_specs=vmem,
            scratch_shapes=[
                pltpu.VMEM((members, rows, width), BF16),
                pltpu.VMEM((members, 2, rows, width), BF16),
                pltpu.VMEM((width, 3 * width), BF16),
                pltpu.VMEM((width, width), BF16),
                pltpu.VMEM((width, inner), BF16),
                pltpu.VMEM((inner, width), BF16),
                pltpu.VMEM((width, width), BF16),
                pltpu.VMEM((width, width), BF16),
                pltpu.VMEM((members, rows, width), BF16),
                pltpu.VMEM((2, 2 * TILE, width), BF16),
                pltpu.VMEM((members, width, rows), BF16),
                pltpu.VMEM((2, HEADS, rows, width // HEADS), BF16),
                pltpu.VMEM((2, width, rows), BF16),
                pltpu.VMEM((members, HEADS, width // HEADS, rows), F32),
                pltpu.VMEM((members, HEADS, 1, rows), F32),
                pltpu.VMEM((members, HEADS, 1, rows), F32),
                pltpu.VMEM((tiles + 2 * RIM_T, rows), F32),
                pltpu.VMEM((HEADS, rows, rows), F32),
                pltpu.VMEM((2, rows // 2, inner), BF16),
                pltpu.VMEM((1, width), F32), pltpu.VMEM((1, width), F32),
                pltpu.SMEM(lists.shape, jnp.int32), pltpu.SMEM(counts.shape, jnp.int32),
                dma((9,)),
                dma((2, members, tiles)), dma((2, members, tiles)),
                dma((4,)), dma((4,)),
            ] + [dma((n_pieces,)) for _ in range(8)],
            compiler_params=pltpu.CompilerParams(
                collective_id=0, has_side_effects=True, vmem_limit_bytes=60 * 1024 * 1024
            ),
        )(
            states, projection, output_w, up_w, down_w,
            gain1.reshape(1, width), gain2.reshape(1, width), lists, counts,
        )

    in_specs = (
        P("member", "mesh", None),
        P("member", None),
        P("member", None),
        P("member", None),
        P("member", None),
        P(),
        P(),
        P("mesh", None),
        P("mesh"),
    )
    return jax.shard_map(
        on_device, mesh=mesh, in_specs=in_specs, out_specs=P("member", "mesh", None), check_vma=False
    )
```

```python
import functools
import math

import jax
import jax.numpy as jnp
from jax import lax
from jax.experimental import pallas as pl
from jax.experimental.pallas import tpu as pltpu
from jax.sharding import PartitionSpec as P

HEADS = 4
TILE = 128
RIM_T = 4
HIDDEN_LOW = -1e30
ONES = 16
WEIGHT_TYPE = jnp.float32
MESH = pl.DeviceIdType.MESH
F32 = jnp.float32
BF16 = jnp.bfloat16

SPLIT = ((0, 4), (1, 1), (2, 2), (3, 2))


def normed(values, gain):
    values = values.astype(F32)
    center = values - jnp.mean(values, axis=-1, keepdims=True)
    spread = jnp.mean(center * center, axis=-1, keepdims=True)
    return (center * lax.rsqrt(spread + 1e-05) * gain).astype(BF16)


def dot_nn(a, b):
    return jnp.dot(a, b, preferred_element_type=F32)


def dot_nt(a, b):
    return lax.dot_general(a, b, (((1,), (1,)), ((), ())), preferred_element_type=F32)


def dot_tn(a, b):
    return lax.dot_general(a, b, (((0,), (0,)), ((), ())), preferred_element_type=F32)


def layer_kernel(
    geometry,
    x_hbm, wp_hbm, wo_hbm, wu_hbm, wd_hbm, gain1_hbm, gain2_hbm, lists_hbm, counts_hbm,
    out_ref,
    own, halo, wp, wo, wu, wd, wq_t, wv_t, xn, hn, q_t, kc, v_t, acc, top, bias, scores, hid, blend,
    gain1, gain2, lists, counts,
    loc_sem, halo_send, halo_recv, p_send, p_recv,
    x_send, x_recv, y_send, y_recv, dx_send, dx_recv, dy_send, dy_recv,
):
    n_mesh, n_z, n_x, n_member = geometry
    members, rows, width = x_hbm.shape
    tiles = rows // TILE
    head = width // HEADS
    i = lax.axis_index("mesh")
    m = lax.axis_index("member")
    nxt = (i + 1) % n_mesh
    prv = (i + n_mesh - 1) % n_mesh
    x_lo = (i // n_z) % n_x
    y = i // (n_z * n_x)
    half = y % 2
    plane = n_z * n_x
    cross = (i + n_z - 2 * n_z * x_lo, (m + 2) % n_member)
    mate = (i, m + 1 - 2 * (m % 2))
    y_to = ((i + n_mesh + plane * (2 * x_lo - 1)) % n_mesh, m)
    y_from = ((i + n_mesh - plane * (2 * x_lo - 1)) % n_mesh, m)
    far = (m + 2) % n_member
    mate_far = (mate[1] + 2) % n_member

    barrier = pltpu.get_barrier_semaphore()
    for peer in ((nxt, m), (prv, m), cross, mate, y_to, y_from):
        pl.semaphore_signal(barrier, inc=1, device_id=peer, device_id_type=MESH)

    sources = (wp_hbm, wo_hbm, wu_hbm, wd_hbm)
    fulls = (wp, wo, wu, wd)

    def shard(w, owner):
        r = sources[w].shape[0]
        return fulls[w].at[pl.ds(pl.multiple_of(owner * r, 16), r), :]

    def piece(w, n, k, owner, which):
        r = sources[w].shape[0]
        size = r // 2 // n
        start = owner * r + which * (r // 2) + k * size
        return fulls[w].at[pl.ds(pl.multiple_of(start, 16), size), :]

    loads = [pltpu.make_async_copy(sources[w], shard(w, m), loc_sem.at[w]) for w in range(4)]
    load_x = pltpu.make_async_copy(x_hbm, own, loc_sem.at[4])
    smalls = [
        pltpu.make_async_copy(src, dst, loc_sem.at[5 + k])
        for k, (src, dst) in enumerate(
            ((lists_hbm, lists), (counts_hbm, counts), (gain1_hbm, gain1), (gain2_hbm, gain2))
        )
    ]
    loads[0].start()
    load_x.start()
    for load in loads[1:] + smalls:
        load.start()

    pieces = []
    for w, n in SPLIT:
        for k in range(n):
            pieces.append((w, n, k))

    def remote(src, dst, send, recv, peer):
        return pltpu.make_async_remote_copy(
            src_ref=src, dst_ref=dst, send_sem=send, recv_sem=recv, device_id=peer, device_id_type=MESH
        )

    def halo_copy(side, b, j):
        src = own.at[b, pl.ds(pl.multiple_of(j * TILE, TILE), TILE), :]
        dst = halo.at[b, side, pl.ds(pl.multiple_of(j * TILE, TILE), TILE), :]
        peer = (nxt, m) if side == 0 else (prv, m)
        return remote(src, dst, halo_send.at[side, b, j], halo_recv.at[side, b, j], peer)

    def mate_copy(w, owner):
        return remote(shard(w, owner), shard(w, owner), p_send.at[w], p_recv.at[w], mate)

    def x_copy(p, owner):
        ref = piece(*pieces[p], owner, half)
        return remote(ref, ref, x_send.at[p], x_recv.at[p], cross)

    def y_copy(p, which):
        ref = piece(*pieces[p], far, which)
        return remote(ref, ref, y_send.at[p], y_recv.at[p], y_to)

    def dx_copy(p, owner):
        ref = piece(*pieces[p], owner, half)
        return remote(ref, ref, dx_send.at[p], dx_recv.at[p], mate)

    def dy_copy(p, owner):
        ref = piece(*pieces[p], owner, 1 - half)
        return remote(ref, ref, dy_send.at[p], dy_recv.at[p], mate)

    def pass_x(p):
        x_copy(p, far).wait_recv()
        y_copy(p, half).start()
        dx_copy(p, far).start()

    def pass_y(p):
        y_copy(p, 1 - half).wait_recv()
        dy_copy(p, far).start()

    def arrive(w):
        mate_copy(w, mate[1]).wait_recv()
        for p, entry in enumerate(pieces):
            if entry[0] == w:
                dx_copy(p, mate_far).wait_recv()
                dy_copy(p, mate_far).wait_recv()

    with jax.named_scope("enter"):
        pl.semaphore_wait(barrier, 6)
        loads[0].wait()
    for p, entry in enumerate(pieces):
        if entry[0] == 0:
            x_copy(p, m).start()
    mate_copy(0, m).start()
    load_x.wait()
    for b in range(members):
        for j in range(tiles):
            for side in range(2):
                halo_copy(side, b, j).start()
    for w in range(1, 4):
        loads[w].wait()
        for p, entry in enumerate(pieces):
            if entry[0] == w:
                x_copy(p, m).start()
        mate_copy(w, m).start()
    for small in smalls:
        small.wait()
    first = i * tiles - RIM_T
    all_tiles = n_mesh * tiles
    entries = lists.shape[1]
    locals_ = [[(lists[t, e] - first + all_tiles) % all_tiles for e in range(entries)] for t in range(tiles)]
    for kt in range(tiles + 2 * RIM_T):
        for t in range(tiles):
            hit = jnp.int32(0)
            for e in range(entries):
                used = jnp.logical_and(locals_[t][e] == kt, e < counts[t])
                hit = jnp.where(used, jnp.int32(1), hit)
            level = jnp.where(hit > 0, F32(0), F32(HIDDEN_LOW))
            bias[pl.ds(kt, 1), t * TILE:(t + 1) * TILE] = jnp.full((1, TILE), level, F32)

    def norm_own(k, _):
        b = k // tiles
        at = pl.ds(pl.multiple_of((k % tiles) * TILE, TILE), TILE)
        xn[b, at, :] = normed(own[b, at, :], gain1[...])
        return 0

    with jax.named_scope("norm_own"):
        lax.fori_loop(0, members * tiles, norm_own, 0)

    steps = members * tiles

    def halo_norm(s, slot):
        b, j = s // tiles, s % tiles
        at = pl.ds(pl.multiple_of(j * TILE, TILE), TILE)
        for side in range(2):
            hn[slot, side * TILE:(side + 1) * TILE, :] = normed(halo[b, side, at, :], gain1[...])

    def halo_wait(s):
        for side in range(2):
            halo_copy(side, s // tiles, s % tiles).wait_recv()

    with jax.named_scope("gather"):
        pass_x(0)
        pass_x(1)
        pass_x(2)
        pass_y(0)
        pass_x(3)
        pass_y(1)
        pass_y(2)
        pass_x(4)
        pass_y(3)
        halo_wait(0)
        halo_norm(0, 0)
        pass_x(5)
        arrive(0)
    with jax.named_scope("flip"):
        wq_t[...] = jnp.transpose(wp[:, :width])
        wv_t[...] = jnp.transpose(wp[:, 2 * width:])
    scale = F32(math.log2(math.e) / math.sqrt(head))

    for slot in range(2):
        for h in range(HEADS):
            v_t[slot, h, head:, :] = jnp.ones((ONES, rows), BF16)

    def weights_of(lowered):
        return jnp.exp2(lowered.astype(WEIGHT_TYPE)).astype(BF16)

    def project(source, slot, n):
        keys = dot_nn(source[...], wp[:, width:2 * width]).astype(BF16)
        for h in range(HEADS):
            kc[slot, h, :n, :] = keys[:, h * head:(h + 1) * head]
        values = dot_nt(wv_t[...], source[...]).astype(BF16)
        for h in range(HEADS):
            v_t[slot, h, :head, :n] = values[h * head:(h + 1) * head, :]

    def attend(b, slot, marks, opening):
        n = len(marks) * TILE
        for h in range(HEADS):
            feats = slice(h * head, (h + 1) * head)
            scores[h, :n, :] = dot_nn(kc[slot, h, :n, :], q_t[b, feats, :])
        for h in range(HEADS):
            feats = slice(h * head, (h + 1) * head)
            best = None if opening else top[b, h]
            for k, mark in enumerate(marks):
                high = jnp.max(scores[h, k * TILE:(k + 1) * TILE, :], axis=0, keepdims=True) + mark
                best = high if best is None else jnp.maximum(best, high)
            parts = [
                weights_of(scores[h, k * TILE:(k + 1) * TILE, :] - (best - mark)) for k, mark in enumerate(marks)
            ]
            product = dot_nn(v_t[slot, h, :, :n], jnp.concatenate(parts, axis=0))
            if opening:
                acc[b, h] = product
            else:
                acc[b, h] = acc[b, h] * jnp.exp2(top[b, h] - best) + product
            top[b, h] = best

    def own_project(b):
        q_t[b] = (dot_nt(wq_t[...], xn[b]) * scale).astype(BF16)
        project(xn.at[b], b, rows)

    def own_attend(b):
        attend(b, b, [bias[RIM_T + t:RIM_T + t + 1, :] for t in range(tiles)], True)

    def halo_project(slot):
        project(hn.at[slot], slot, 2 * TILE)

    def halo_attend(s, slot):
        b, j = s // tiles, s % tiles
        attend(b, slot, [bias[pl.ds(j, 1), :], bias[pl.ds(j + RIM_T + tiles, 1), :]], False)

    with jax.named_scope("own0"):
        own_project(0)
    with jax.named_scope("own1"):
        own_attend(0)
        own_project(1)
    pass_x(6)
    pass_y(4)
    with jax.named_scope("wait1"):
        halo_wait(1)
    with jax.named_scope("own2"):
        own_attend(1)
        halo_project(0)
        halo_norm(1, 1)

    def two_steps(t, _):
        s = 2 * t
        with jax.named_scope("wait2"):
            halo_wait(s + 2)

            @pl.when(t == 0)
            def _():
                pass_y(5)
                pass_x(7)

            @pl.when(t == 1)
            def _():
                pass_y(6)

            @pl.when(t == 2)
            def _():
                pass_y(7)

        with jax.named_scope("stepa"):
            halo_attend(s, 0)
            halo_project(1)
            halo_norm(s + 2, 0)
        with jax.named_scope("wait3"):
            halo_wait(s + 3)

            @pl.when(t == 0)
            def _():
                pass_x(8)

            @pl.when(t == 2)
            def _():
                pass_y(8)

        with jax.named_scope("stepb"):
            halo_attend(s + 1, 1)
            halo_project(0)
            halo_norm(s + 3, 1)
        return 0

    lax.fori_loop(0, steps // 2 - 1, two_steps, 0)
    with jax.named_scope("last"):
        halo_attend(steps - 2, 0)
        halo_project(1)
        halo_attend(steps - 1, 1)
    with jax.named_scope("gather2"):
        arrive(1)
        arrive(2)
        arrive(3)

    block = rows // 2
    inner = wu.shape[1]
    step = inner // 4
    slope = math.sqrt(2.0 / math.pi)

    def residual(b, r):
        at = slice(r * block, (r + 1) * block)
        return (own[b, at, :].astype(F32) + dot_tn(blend[b, :, at], wo[...])).astype(BF16)

    def feed(b, r, middle):
        at = slice(r * block, (r + 1) * block)
        second = normed(middle, gain2[...])
        for f in range(4):
            u = dot_nn(second, wu[:, f * step:(f + 1) * step])
            bent = jnp.tanh(u * (slope + (slope * 0.044715) * (u * u)))
            hid[r, :, f * step:(f + 1) * step] = (u + u * bent).astype(BF16)
        out_ref[b, at, :] = (middle.astype(F32) + 0.5 * dot_nn(hid[r], wd[...])).astype(BF16)

    with jax.named_scope("finish"):
        for b in range(members):
            for h in range(HEADS):
                inverse = 1.0 / acc[b, h, head:head + 1, :]
                blend[b, h * head:(h + 1) * head, :] = (acc[b, h, :head, :] * inverse).astype(BF16)
        jobs = [(b, r) for b in range(members) for r in range(2)]
        middle = residual(*jobs[0])
        for k, job in enumerate(jobs):
            later = residual(*jobs[k + 1]) if k + 1 < len(jobs) else None
            feed(*job, middle)
            middle = later

    for b in range(members):
        for j in range(tiles):
            for side in range(2):
                halo_copy(side, b, j).wait_send()
    for w in range(4):
        mate_copy(w, m).wait_send()
    for p in range(len(pieces)):
        x_copy(p, m).wait_send()
        y_copy(p, half).wait_send()
        dx_copy(p, far).wait_send()
        dy_copy(p, far).wait_send()


def solution(mesh):
    n_mesh, n_member = mesh.shape["mesh"], mesh.shape["member"]
    geometry = (n_mesh, 4, 2, n_member)

    def on_device(states, projection, output_w, up_w, down_w, gain1, gain2, lists, counts):
        members, rows, width = states.shape
        inner = up_w.shape[1]
        tiles = rows // TILE
        n_pieces = sum(n for _, n in SPLIT)
        hbm = pl.BlockSpec(memory_space=pl.ANY)
        vmem = pl.BlockSpec(memory_space=pltpu.VMEM)
        dma = pltpu.SemaphoreType.DMA
        return pl.pallas_call(
            functools.partial(layer_kernel, geometry),
            name="layer",
            out_shape=pltpu.VMEM(states.shape, BF16),
            in_specs=[hbm] * 9,
            out_specs=vmem,
            scratch_shapes=[
                pltpu.VMEM((members, rows, width), BF16),
                pltpu.VMEM((members, 2, rows, width), BF16),
                pltpu.VMEM((width, 3 * width), BF16),
                pltpu.VMEM((width, width), BF16),
                pltpu.VMEM((width, inner), BF16),
                pltpu.VMEM((inner, width), BF16),
                pltpu.VMEM((width, width), BF16),
                pltpu.VMEM((width, width), BF16),
                pltpu.VMEM((members, rows, width), BF16),
                pltpu.VMEM((2, 2 * TILE, width), BF16),
                pltpu.VMEM((members, width, rows), BF16),
                pltpu.VMEM((2, HEADS, rows, width // HEADS), BF16),
                pltpu.VMEM((2, HEADS, width // HEADS + ONES, rows), BF16),
                pltpu.VMEM((members, HEADS, width // HEADS + ONES, rows), F32),
                pltpu.VMEM((members, HEADS, 1, rows), F32),
                pltpu.VMEM((tiles + 2 * RIM_T, rows), F32),
                pltpu.VMEM((HEADS, rows, rows), F32),
                pltpu.VMEM((2, rows // 2, inner), BF16),
                pltpu.VMEM((members, width, rows), BF16),
                pltpu.VMEM((1, width), F32), pltpu.VMEM((1, width), F32),
                pltpu.SMEM(lists.shape, jnp.int32), pltpu.SMEM(counts.shape, jnp.int32),
                dma((9,)),
                dma((2, members, tiles)), dma((2, members, tiles)),
                dma((4,)), dma((4,)),
            ] + [dma((n_pieces,)) for _ in range(8)],
            compiler_params=pltpu.CompilerParams(
                collective_id=0, has_side_effects=True, vmem_limit_bytes=60 * 1024 * 1024
            ),
        )(
            states, projection, output_w, up_w, down_w,
            gain1.reshape(1, width), gain2.reshape(1, width), lists, counts,
        )

    in_specs = (
        P("member", "mesh", None),
        P("member", None),
        P("member", None),
        P("member", None),
        P("member", None),
        P(),
        P(),
        P("mesh", None),
        P("mesh"),
    )
    return jax.shard_map(
        on_device, mesh=mesh, in_specs=in_specs, out_specs=P("member", "mesh", None), check_vma=False
    )
```

```python
import functools
import math

import jax
import jax.numpy as jnp
from jax import lax
from jax.experimental import pallas as pl
from jax.experimental.pallas import tpu as pltpu
from jax.sharding import PartitionSpec as P

HEADS = 4
TILE = 128
RIM_T = 4
HIDDEN_LOW = -1e30
ONES = 16
WEIGHT_TYPE = jnp.float32
MESH = pl.DeviceIdType.MESH
F32 = jnp.float32
BF16 = jnp.bfloat16

SPLIT = ((0, 2), (1, 2), (2, 2), (3, 1), (4, 2), (5, 4))
KEYS, VALUES, QUERIES, OUTPUT, UP, DOWN = range(6)


def normed(values, gain):
    values = values.astype(F32)
    center = values - jnp.mean(values, axis=-1, keepdims=True)
    spread = jnp.mean(center * center, axis=-1, keepdims=True)
    return (center * lax.rsqrt(spread + 1e-05) * gain).astype(BF16)


def dot_nn(a, b):
    return jnp.dot(a, b, preferred_element_type=F32)


def dot_nt(a, b):
    return lax.dot_general(a, b, (((1,), (1,)), ((), ())), preferred_element_type=F32)


def dot_tn(a, b):
    return lax.dot_general(a, b, (((0,), (0,)), ((), ())), preferred_element_type=F32)


def layer_kernel(
    geometry,
    x_hbm, wp_hbm, wo_hbm, wu_hbm, wd_hbm, gain1_hbm, gain2_hbm, lists_hbm, counts_hbm,
    out_ref,
    own, halo, wk, wv, wq, wo, wu, wd, wq_t, wv_t, xn, hn, q_t, kc, v_t, acc, top, bias, scores, hid, blend,
    second, mid,
    gain1, gain2, lists, counts,
    loc_sem, halo_send, halo_recv, p_send, p_recv,
    x_send, x_recv, y_send, y_recv, dx_send, dx_recv, dy_send, dy_recv,
):
    n_mesh, n_z, n_x, n_member = geometry
    members, rows, width = x_hbm.shape
    tiles = rows // TILE
    head = width // HEADS
    i = lax.axis_index("mesh")
    m = lax.axis_index("member")
    nxt = (i + 1) % n_mesh
    prv = (i + n_mesh - 1) % n_mesh
    x_lo = (i // n_z) % n_x
    y = i // (n_z * n_x)
    half = y % 2
    plane = n_z * n_x
    cross = (i + n_z - 2 * n_z * x_lo, (m + 2) % n_member)
    mate = (i, m + 1 - 2 * (m % 2))
    y_to = ((i + n_mesh + plane * (2 * x_lo - 1)) % n_mesh, m)
    y_from = ((i + n_mesh - plane * (2 * x_lo - 1)) % n_mesh, m)
    far = (m + 2) % n_member
    mate_far = (mate[1] + 2) % n_member

    barrier = pltpu.get_barrier_semaphore()
    for peer in ((nxt, m), (prv, m), cross, mate, y_to, y_from):
        pl.semaphore_signal(barrier, inc=1, device_id=peer, device_id_type=MESH)

    sources = (
        wp_hbm.at[:, pl.ds(width, width)], wp_hbm.at[:, pl.ds(2 * width, width)], wp_hbm.at[:, pl.ds(0, width)],
        wo_hbm, wu_hbm, wd_hbm,
    )
    fulls = (wk, wv, wq, wo, wu, wd)
    n_weights = len(fulls)

    def shard(w, owner):
        r = sources[w].shape[0]
        return fulls[w].at[pl.ds(pl.multiple_of(owner * r, 16), r), :]

    def piece(w, n, k, owner, which):
        r = sources[w].shape[0]
        size = r // 2 // n
        start = owner * r + which * (r // 2) + k * size
        return fulls[w].at[pl.ds(pl.multiple_of(start, 16), size), :]

    loads = [pltpu.make_async_copy(sources[w], shard(w, m), loc_sem.at[w]) for w in range(n_weights)]
    load_x = pltpu.make_async_copy(x_hbm, own, loc_sem.at[n_weights])
    smalls = [
        pltpu.make_async_copy(src, dst, loc_sem.at[n_weights + 1 + k])
        for k, (src, dst) in enumerate(
            ((lists_hbm, lists), (counts_hbm, counts), (gain1_hbm, gain1), (gain2_hbm, gain2))
        )
    ]
    for load in loads[:3] + [load_x] + loads[3:] + smalls:
        load.start()

    pieces = []
    for w, n in SPLIT:
        for k in range(n):
            pieces.append((w, n, k))

    def remote(src, dst, send, recv, peer):
        return pltpu.make_async_remote_copy(
            src_ref=src, dst_ref=dst, send_sem=send, recv_sem=recv, device_id=peer, device_id_type=MESH
        )

    def halo_copy(side, b, j):
        src = own.at[b, pl.ds(pl.multiple_of(j * TILE, TILE), TILE), :]
        dst = halo.at[b, side, pl.ds(pl.multiple_of(j * TILE, TILE), TILE), :]
        peer = (nxt, m) if side == 0 else (prv, m)
        return remote(src, dst, halo_send.at[side, b, j], halo_recv.at[side, b, j], peer)

    def mate_copy(w, owner):
        return remote(shard(w, owner), shard(w, owner), p_send.at[w], p_recv.at[w], mate)

    def x_copy(p, owner):
        ref = piece(*pieces[p], owner, half)
        return remote(ref, ref, x_send.at[p], x_recv.at[p], cross)

    def y_copy(p, which):
        ref = piece(*pieces[p], far, which)
        return remote(ref, ref, y_send.at[p], y_recv.at[p], y_to)

    def dx_copy(p, owner):
        ref = piece(*pieces[p], owner, half)
        return remote(ref, ref, dx_send.at[p], dx_recv.at[p], mate)

    def dy_copy(p, owner):
        ref = piece(*pieces[p], owner, 1 - half)
        return remote(ref, ref, dy_send.at[p], dy_recv.at[p], mate)

    def pass_x(p):
        x_copy(p, far).wait_recv()
        y_copy(p, half).start()
        dx_copy(p, far).start()

    def pass_y(p):
        y_copy(p, 1 - half).wait_recv()
        dy_copy(p, far).start()

    def arrive(w):
        mate_copy(w, mate[1]).wait_recv()
        for p, entry in enumerate(pieces):
            if entry[0] == w:
                dx_copy(p, mate_far).wait_recv()
                dy_copy(p, mate_far).wait_recv()

    def send_weight(w):
        loads[w].wait()
        for p, entry in enumerate(pieces):
            if entry[0] == w:
                x_copy(p, m).start()
        mate_copy(w, m).start()

    with jax.named_scope("enter"):
        pl.semaphore_wait(barrier, 6)
    send_weight(KEYS)
    send_weight(VALUES)
    send_weight(QUERIES)
    load_x.wait()
    for b in range(members):
        for j in range(tiles):
            for side in range(2):
                halo_copy(side, b, j).start()
    send_weight(OUTPUT)
    send_weight(UP)
    send_weight(DOWN)
    for small in smalls:
        small.wait()
    first = i * tiles - RIM_T
    all_tiles = n_mesh * tiles
    entries = lists.shape[1]
    locals_ = [[(lists[t, e] - first + all_tiles) % all_tiles for e in range(entries)] for t in range(tiles)]
    for kt in range(tiles + 2 * RIM_T):
        for t in range(tiles):
            hit = jnp.int32(0)
            for e in range(entries):
                used = jnp.logical_and(locals_[t][e] == kt, e < counts[t])
                hit = jnp.where(used, jnp.int32(1), hit)
            level = jnp.where(hit > 0, F32(0), F32(HIDDEN_LOW))
            bias[pl.ds(kt, 1), t * TILE:(t + 1) * TILE] = jnp.full((1, TILE), level, F32)

    def norm_own(k, _):
        b = k // tiles
        at = pl.ds(pl.multiple_of((k % tiles) * TILE, TILE), TILE)
        xn[b, at, :] = normed(own[b, at, :], gain1[...])
        return 0

    with jax.named_scope("norm_own"):
        lax.fori_loop(0, members * tiles, norm_own, 0)

    steps = members * tiles

    def halo_norm(s, slot):
        b, j = s // tiles, s % tiles
        at = pl.ds(pl.multiple_of(j * TILE, TILE), TILE)
        for side in range(2):
            hn[slot, side * TILE:(side + 1) * TILE, :] = normed(halo[b, side, at, :], gain1[...])

    def halo_wait(s):
        for side in range(2):
            halo_copy(side, s // tiles, s % tiles).wait_recv()

    scale = F32(math.log2(math.e) / math.sqrt(head))

    for slot in range(3):
        for h in range(HEADS):
            v_t[slot, h, head:, :] = jnp.ones((ONES, rows), BF16)

    def weights_of(lowered):
        return jnp.exp2(lowered.astype(WEIGHT_TYPE)).astype(BF16)

    def project_keys(source, slot, n):
        keys = dot_nn(source[...], wk[...]).astype(BF16)
        for h in range(HEADS):
            kc[slot, h, :n, :] = keys[:, h * head:(h + 1) * head]

    def project_values(source, slot, n):
        values = dot_nt(wv_t[...], source[...]).astype(BF16)
        for h in range(HEADS):
            v_t[slot, h, :head, :n] = values[h * head:(h + 1) * head, :]

    def project_queries(b):
        q_t[b] = (dot_nt(wq_t[...], xn[b]) * scale).astype(BF16)

    def attend(b, slot, marks, opening):
        n = len(marks) * TILE
        for h in range(HEADS):
            feats = slice(h * head, (h + 1) * head)
            scores[h, :n, :] = dot_nn(kc[slot, h, :n, :], q_t[b, feats, :])
        for h in range(HEADS):
            feats = slice(h * head, (h + 1) * head)
            best = None if opening else top[b, h]
            for k, mark in enumerate(marks):
                high = jnp.max(scores[h, k * TILE:(k + 1) * TILE, :], axis=0, keepdims=True) + mark
                best = high if best is None else jnp.maximum(best, high)
            parts = [
                weights_of(scores[h, k * TILE:(k + 1) * TILE, :] - (best - mark)) for k, mark in enumerate(marks)
            ]
            product = dot_nn(v_t[slot, h, :, :n], jnp.concatenate(parts, axis=0))
            if opening:
                acc[b, h] = product
            else:
                acc[b, h] = acc[b, h] * jnp.exp2(top[b, h] - best) + product
            top[b, h] = best

    def own_attend(b):
        attend(b, 1 + b, [bias[RIM_T + t:RIM_T + t + 1, :] for t in range(tiles)], True)

    def halo_project(s):
        project_keys(hn.at[s % 2], s % 2, 2 * TILE)
        project_values(hn.at[s % 2], s % 2, 2 * TILE)

    def halo_attend(s):
        b, j = s // tiles, s % tiles
        attend(b, s % 2, [bias[j:j + 1, :], bias[j + RIM_T + tiles:j + RIM_T + tiles + 1, :]], False)

    block = rows // 2
    inner = wu.shape[1]
    step = inner // 4
    slope = math.sqrt(2.0 / math.pi)

    def merge(b):
        for h in range(HEADS):
            inverse = 1.0 / acc[b, h, head:head + 1, :]
            blend[h * head:(h + 1) * head, :] = (acc[b, h, :head, :] * inverse).astype(BF16)

    def residual(b, r):
        at = slice(r * block, (r + 1) * block)
        middle = (own[b, at, :].astype(F32) + dot_tn(blend[:, at], wo[...])).astype(BF16)
        mid[r] = middle
        second[r] = normed(middle, gain2[...])

    def rise(r):
        for f in range(4):
            u = dot_nn(second[r], wu[:, f * step:(f + 1) * step])
            bent = jnp.tanh(u * (slope + (slope * 0.044715) * (u * u)))
            hid[r, :, f * step:(f + 1) * step] = (u + u * bent).astype(BF16)

    def fall(b, r):
        at = slice(r * block, (r + 1) * block)
        out_ref[b, at, :] = (mid[r].astype(F32) + 0.5 * dot_nn(hid[r], wd[...])).astype(BF16)

    index = {}
    for p, entry in enumerate(pieces):
        index[(entry[0], entry[2])] = p

    def px(w, k):
        with jax.named_scope(f"px{w}{k}"):
            pass_x(index[(w, k)])

    def py(w, k):
        with jax.named_scope(f"py{w}{k}"):
            pass_y(index[(w, k)])

    def have(w):
        with jax.named_scope(f"have{w}"):
            arrive(w)

    def halo_ready(s):
        with jax.named_scope(f"halo{s}"):
            halo_wait(s)

    px(KEYS, 0)
    px(KEYS, 1)
    px(VALUES, 0)
    px(VALUES, 1)
    py(KEYS, 0)
    px(QUERIES, 0)
    py(KEYS, 1)
    px(QUERIES, 1)
    py(VALUES, 0)
    have(KEYS)
    with jax.named_scope("keys"):
        for b in range(members):
            project_keys(xn.at[b], 1 + b, rows)
    py(VALUES, 1)
    px(OUTPUT, 0)
    py(QUERIES, 0)
    have(VALUES)
    with jax.named_scope("values"):
        wv_t[...] = jnp.transpose(wv[...])
        for b in range(members):
            project_values(xn.at[b], 1 + b, rows)
    py(QUERIES, 1)
    halo_ready(0)
    have(QUERIES)
    with jax.named_scope("queries"):
        wq_t[...] = jnp.transpose(wq[...])
        project_queries(0)
        halo_norm(0, 0)
    px(UP, 0)
    halo_ready(1)
    with jax.named_scope("own0"):
        own_attend(0)
        project_queries(1)
        halo_project(0)
    py(OUTPUT, 0)
    px(UP, 1)
    with jax.named_scope("own1"):
        own_attend(1)
        halo_norm(1, 1)
    halo_ready(2)
    px(DOWN, 0)
    with jax.named_scope("s0"):
        halo_attend(0)
        halo_project(1)
        halo_norm(2, 0)
    halo_ready(3)
    py(UP, 0)
    px(DOWN, 1)
    with jax.named_scope("s1"):
        halo_attend(1)
        halo_project(2)
        halo_norm(3, 1)
    halo_ready(4)
    with jax.named_scope("s2"):
        halo_attend(2)
        halo_project(3)
        halo_norm(4, 0)
    px(DOWN, 2)
    py(UP, 1)
    with jax.named_scope("s3"):
        halo_attend(3)
        merge(0)
        halo_project(4)
    px(DOWN, 3)
    py(DOWN, 0)
    have(OUTPUT)
    halo_ready(5)
    with jax.named_scope("s4"):
        residual(0, 0)
        residual(0, 1)
        halo_attend(4)
        halo_norm(5, 1)
    py(DOWN, 1)
    have(UP)
    halo_ready(6)
    with jax.named_scope("s5"):
        rise(0)
        halo_project(5)
        halo_attend(5)
        halo_norm(6, 0)
    py(DOWN, 2)
    with jax.named_scope("s6"):
        rise(1)
        halo_project(6)
        halo_attend(6)
    py(DOWN, 3)
    halo_ready(7)
    with jax.named_scope("s7a"):
        halo_norm(7, 1)
        halo_project(7)
    have(DOWN)
    with jax.named_scope("s7b"):
        halo_attend(7)
        fall(0, 0)
        fall(0, 1)
        merge(1)
    with jax.named_scope("finish"):
        residual(1, 0)
        rise(0)
        residual(1, 1)
        fall(1, 0)
        rise(1)
        fall(1, 1)

    for b in range(members):
        for j in range(tiles):
            for side in range(2):
                halo_copy(side, b, j).wait_send()
    for w in range(n_weights):
        mate_copy(w, m).wait_send()
    for p in range(len(pieces)):
        x_copy(p, m).wait_send()
        y_copy(p, half).wait_send()
        dx_copy(p, far).wait_send()
        dy_copy(p, far).wait_send()


def solution(mesh):
    n_mesh, n_member = mesh.shape["mesh"], mesh.shape["member"]
    geometry = (n_mesh, 4, 2, n_member)

    def on_device(states, projection, output_w, up_w, down_w, gain1, gain2, lists, counts):
        members, rows, width = states.shape
        inner = up_w.shape[1]
        tiles = rows // TILE
        n_pieces = sum(n for _, n in SPLIT)
        hbm = pl.BlockSpec(memory_space=pl.ANY)
        vmem = pl.BlockSpec(memory_space=pltpu.VMEM)
        dma = pltpu.SemaphoreType.DMA
        return pl.pallas_call(
            functools.partial(layer_kernel, geometry),
            name="layer",
            out_shape=pltpu.VMEM(states.shape, BF16),
            in_specs=[hbm] * 9,
            out_specs=vmem,
            scratch_shapes=[
                pltpu.VMEM((members, rows, width), BF16),
                pltpu.VMEM((members, 2, rows, width), BF16),
                pltpu.VMEM((width, width), BF16),
                pltpu.VMEM((width, width), BF16),
                pltpu.VMEM((width, width), BF16),
                pltpu.VMEM((width, width), BF16),
                pltpu.VMEM((width, inner), BF16),
                pltpu.VMEM((inner, width), BF16),
                pltpu.VMEM((width, width), BF16),
                pltpu.VMEM((width, width), BF16),
                pltpu.VMEM((members, rows, width), BF16),
                pltpu.VMEM((2, 2 * TILE, width), BF16),
                pltpu.VMEM((members, width, rows), BF16),
                pltpu.VMEM((3, HEADS, rows, width // HEADS), BF16),
                pltpu.VMEM((3, HEADS, width // HEADS + ONES, rows), BF16),
                pltpu.VMEM((members, HEADS, width // HEADS + ONES, rows), F32),
                pltpu.VMEM((members, HEADS, 1, rows), F32),
                pltpu.VMEM((tiles + 2 * RIM_T, rows), F32),
                pltpu.VMEM((HEADS, rows, rows), F32),
                pltpu.VMEM((2, rows // 2, inner), BF16),
                pltpu.VMEM((width, rows), BF16),
                pltpu.VMEM((2, rows // 2, width), BF16),
                pltpu.VMEM((2, rows // 2, width), BF16),
                pltpu.VMEM((1, width), F32), pltpu.VMEM((1, width), F32),
                pltpu.SMEM(lists.shape, jnp.int32), pltpu.SMEM(counts.shape, jnp.int32),
                dma((11,)),
                dma((2, members, tiles)), dma((2, members, tiles)),
                dma((6,)), dma((6,)),
            ] + [dma((n_pieces,)) for _ in range(8)],
            compiler_params=pltpu.CompilerParams(
                collective_id=0, has_side_effects=True, vmem_limit_bytes=60 * 1024 * 1024
            ),
        )(
            states, projection, output_w, up_w, down_w,
            gain1.reshape(1, width), gain2.reshape(1, width), lists, counts,
        )

    in_specs = (
        P("member", "mesh", None),
        P("member", None),
        P("member", None),
        P("member", None),
        P("member", None),
        P(),
        P(),
        P("mesh", None),
        P("mesh"),
    )
    return jax.shard_map(
        on_device, mesh=mesh, in_specs=in_specs, out_specs=P("member", "mesh", None), check_vma=False
    )
```

```python
import functools
import math

import jax
import jax.numpy as jnp
from jax import lax
from jax.experimental import pallas as pl
from jax.experimental.pallas import tpu as pltpu
from jax.sharding import PartitionSpec as P

HEADS = 4
TILE = 128
RIM_T = 4
HIDDEN_LOW = -1e30
ONES = 16
AHEAD = 4
MESH = pl.DeviceIdType.MESH
F32 = jnp.float32
BF16 = jnp.bfloat16

SPLIT = ((0, 2), (1, 2), (2, 2), (3, 1), (4, 2), (5, 4))
KEYS, VALUES, QUERIES, OUTPUT, UP, DOWN = range(6)


def normed(values, gain):
    values = values.astype(F32)
    center = values - jnp.mean(values, axis=-1, keepdims=True)
    spread = jnp.mean(center * center, axis=-1, keepdims=True)
    return (center * lax.rsqrt(spread + 1e-05) * gain).astype(BF16)


def dot_nn(a, b):
    return jnp.dot(a, b, preferred_element_type=F32)


def dot_nt(a, b):
    return lax.dot_general(a, b, (((1,), (1,)), ((), ())), preferred_element_type=F32)


def dot_tn(a, b):
    return lax.dot_general(a, b, (((0,), (0,)), ((), ())), preferred_element_type=F32)


def layer_kernel(
    geometry,
    x_hbm, wp_hbm, wo_hbm, wu_hbm, wd_hbm, gain1_hbm, gain2_hbm, lists_hbm, counts_hbm,
    out_ref,
    own, halo, wk, wv, wq, wo, wu, wd, wq_t, wv_t, xn, hn, q_t, kc, v_t, acc, top, bias, scores, hid, blend,
    second, mid,
    gain1, gain2, lists, counts,
    loc_sem, halo_send, halo_recv, weight_send, mate_recv, x_recv, y_recv,
):
    n_mesh, n_z, n_x, n_member = geometry
    members, rows, width = x_hbm.shape
    tiles = rows // TILE
    head = width // HEADS
    i = lax.axis_index("mesh")
    m = lax.axis_index("member")
    nxt = (i + 1) % n_mesh
    prv = (i + n_mesh - 1) % n_mesh
    x_lo = (i // n_z) % n_x
    y = i // (n_z * n_x)
    half = y % 2
    plane = n_z * n_x
    cross = (i + n_z - 2 * n_z * x_lo, (m + 2) % n_member)
    mate = (i, m + 1 - 2 * (m % 2))
    y_to = ((i + n_mesh + plane * (2 * x_lo - 1)) % n_mesh, m)
    y_from = ((i + n_mesh - plane * (2 * x_lo - 1)) % n_mesh, m)
    far = (m + 2) % n_member
    mate_far = (mate[1] + 2) % n_member

    barrier = pltpu.get_barrier_semaphore()
    for peer in ((nxt, m), (prv, m), cross, mate, y_to, y_from):
        pl.semaphore_signal(barrier, inc=1, device_id=peer, device_id_type=MESH)

    sources = (
        wp_hbm.at[:, pl.ds(width, width)], wp_hbm.at[:, pl.ds(2 * width, width)], wp_hbm.at[:, pl.ds(0, width)],
        wo_hbm, wu_hbm, wd_hbm,
    )
    fulls = (wk, wv, wq, wo, wu, wd)
    n_weights = len(fulls)

    def shard(w, owner):
        r = sources[w].shape[0]
        return fulls[w].at[pl.ds(pl.multiple_of(owner * r, 16), r), :]

    def piece(w, n, k, owner, which):
        r = sources[w].shape[0]
        size = r // 2 // n
        start = owner * r + which * (r // 2) + k * size
        return fulls[w].at[pl.ds(pl.multiple_of(start, 16), size), :]

    loads = [pltpu.make_async_copy(sources[w], shard(w, m), loc_sem.at[w]) for w in range(n_weights)]
    spots = [(0, slice(0, TILE)), (0, slice(TILE, rows)), (1, slice(0, rows))]
    load_x = [
        pltpu.make_async_copy(x_hbm.at[b, at, :], own.at[b, at, :], loc_sem.at[n_weights + 5 + k])
        for k, (b, at) in enumerate(spots)
    ]
    smalls = [
        pltpu.make_async_copy(src, dst, loc_sem.at[n_weights + 1 + k])
        for k, (src, dst) in enumerate(
            ((lists_hbm, lists), (counts_hbm, counts), (gain1_hbm, gain1), (gain2_hbm, gain2))
        )
    ]
    for load in load_x[:1] + loads[:3] + load_x[1:] + loads[3:] + smalls:
        load.start()

    pieces = []
    for w, n in SPLIT:
        for k in range(n):
            pieces.append((w, n, k))

    def remote(src, dst, send, recv, peer):
        return pltpu.make_async_remote_copy(
            src_ref=src, dst_ref=dst, send_sem=send, recv_sem=recv, device_id=peer, device_id_type=MESH
        )

    def halo_copy(side, b, j):
        raw = b == 0 and j == 0
        src = (own if raw else xn).at[b, pl.ds(j * TILE, TILE), :]
        dst = halo.at[b, j, pl.ds(side * TILE, TILE), :]
        peer = (nxt, m) if side == 0 else (prv, m)
        return remote(src, dst, halo_send.at[0], halo_recv.at[tiles * b + j], peer)

    def mate_copy(w, owner):
        return remote(shard(w, owner), shard(w, owner), weight_send.at[w], mate_recv.at[w], mate)

    def x_copy(p, owner):
        ref = piece(*pieces[p], owner, half)
        return remote(ref, ref, weight_send.at[pieces[p][0]], x_recv.at[p], cross)

    def y_copy(p, which):
        ref = piece(*pieces[p], far, which)
        return remote(ref, ref, weight_send.at[pieces[p][0]], y_recv.at[p], y_to)

    def d_copy(p, which):
        ref = piece(*pieces[p], far, which)
        return remote(ref, ref, weight_send.at[pieces[p][0]], mate_recv.at[pieces[p][0]], mate)

    def pass_x(p):
        x_copy(p, far).wait_recv()
        y_copy(p, half).start()
        d_copy(p, half).start()

    def pass_y(p):
        y_copy(p, 1 - half).wait_recv()
        d_copy(p, 1 - half).start()

    def arrive(w):
        both = fulls[w].at[pl.ds(0, 2 * sources[w].shape[0]), :]
        remote(both, both, weight_send.at[w], mate_recv.at[w], mate).wait_recv()

    def send_weight(w):
        loads[w].wait()
        for p, entry in enumerate(pieces):
            if entry[0] == w:
                x_copy(p, m).start()
        mate_copy(w, m).start()

    with jax.named_scope("enter"):
        pl.semaphore_wait(barrier, 6)
    load_x[0].wait()
    for side in range(2):
        halo_copy(side, 0, 0).start()
    send_weight(KEYS)
    send_weight(VALUES)
    send_weight(QUERIES)
    load_x[1].wait()
    load_x[2].wait()
    def norm_own(k, _):
        b = k // tiles
        at = pl.ds(pl.multiple_of((k % tiles) * TILE, TILE), TILE)
        xn[b, at, :] = normed(own[b, at, :], gain1[...])
        return 0

    with jax.named_scope("norm_own"):
        smalls[2].wait()
        smalls[3].wait()
        for b in range(members):
            lax.fori_loop(b * tiles, (b + 1) * tiles, norm_own, 0)
            for j in range(tiles):
                if b + j > 0:
                    for side in range(2):
                        halo_copy(side, b, j).start()
        send_weight(OUTPUT)
        send_weight(UP)
        send_weight(DOWN)
    for small in smalls[:2]:
        small.wait()
    first = i * tiles - RIM_T
    all_tiles = n_mesh * tiles
    entries = lists.shape[1]
    locals_ = [[(lists[t, e] - first + all_tiles) % all_tiles for e in range(entries)] for t in range(tiles)]
    for kt in range(tiles + 2 * RIM_T):
        for t in range(tiles):
            hit = jnp.int32(0)
            for e in range(entries):
                used = jnp.logical_and(locals_[t][e] == kt, e < counts[t])
                hit = jnp.where(used, jnp.int32(1), hit)
            level = jnp.where(hit > 0, F32(0), F32(HIDDEN_LOW))
            bias[pl.ds(kt, 1), t * TILE:(t + 1) * TILE] = jnp.full((1, TILE), level, F32)


    steps = members * tiles

    def norm_first(k):
        part = slice(k * (TILE // 2), (k + 1) * (TILE // 2))
        hn[part, :] = normed(halo[0, 0, part, :], gain1[...])

    first_jobs = [functools.partial(norm_first, k) for k in range(4)]

    def halo_wait(s):
        chunk = halo.at[s // tiles, s % tiles]
        remote(chunk, chunk, halo_send.at[0], halo_recv.at[s], (nxt, m)).wait_recv()

    scale = F32(math.log2(math.e) / math.sqrt(head))

    for slot in range(3):
        for h in range(HEADS):
            v_t[slot, h, head:, :] = jnp.ones((ONES, rows), BF16)

    wide = 2 * TILE
    spans = [slice(c * wide, (c + 1) * wide) for c in range(width // wide)]

    def key_jobs(source, slot, n):
        def job(span):
            keys = dot_nn(source[...], wk[:, span]).astype(BF16)
            for k in range(wide // head):
                kc[slot, span.start // head + k, :n, :] = keys[:, k * head:(k + 1) * head]

        return [functools.partial(job, span) for span in spans]

    def value_jobs(source, slot, n):
        def job(span):
            values = dot_nt(wv_t[span, :], source[...]).astype(BF16)
            for k in range(wide // head):
                v_t[slot, span.start // head + k, :head, :n] = values[k * head:(k + 1) * head, :]

        return [functools.partial(job, span) for span in spans]

    def query_jobs(b):
        def job(span):
            q_t[b, span, :] = (dot_nt(wq_t[span, :], xn[b]) * scale).astype(BF16)

        return [functools.partial(job, span) for span in spans]

    def attend_jobs(b, slot, marks, opening):
        n = len(marks) * TILE
        blocks = [(h, cols) for h in range(HEADS) for cols in spans]

        def score(h, cols):
            feats = slice(h * head, (h + 1) * head)
            scores[h, :n, cols] = dot_nn(kc[slot, h, :n, :], q_t[b, feats, cols])

        def blend_in(h, cols):
            best = None if opening else top[b, h, :, cols]
            for k, mark in enumerate(marks):
                high = jnp.max(scores[h, k * TILE:(k + 1) * TILE, cols], axis=0, keepdims=True) + mark[:, cols]
                best = high if best is None else jnp.maximum(best, high)
            parts = [
                jnp.exp2(scores[h, k * TILE:(k + 1) * TILE, cols] - (best - mark[:, cols])).astype(BF16)
                for k, mark in enumerate(marks)
            ]
            product = dot_nn(v_t[slot, h, :, :n], jnp.concatenate(parts, axis=0))
            if opening:
                acc[b, h, :, cols] = product
            else:
                acc[b, h, :, cols] = acc[b, h, :, cols] * jnp.exp2(top[b, h, :, cols] - best) + product
            top[b, h, :, cols] = best

        def job(k):
            if k == 0:
                for block in blocks[:AHEAD]:
                    score(*block)
            if k + AHEAD < len(blocks):
                score(*blocks[k + AHEAD])
            blend_in(*blocks[k])

        return [functools.partial(job, k) for k in range(len(blocks))]

    def own_jobs(b):
        return attend_jobs(b, 1 + b, [bias[RIM_T + t:RIM_T + t + 1, :] for t in range(tiles)], True)

    def project_jobs(s):
        source, slot = hn if s == 0 else halo.at[s // tiles, s % tiles], s % 2
        return key_jobs(source, slot, 2 * TILE) + value_jobs(source, slot, 2 * TILE)

    def halo_jobs(s):
        b, j = s // tiles, s % tiles
        return attend_jobs(b, s % 2, [bias[j:j + 1, :], bias[j + RIM_T + tiles:j + RIM_T + tiles + 1, :]], False)

    block_rows = rows // 2
    inner = wu.shape[1]
    slope = math.sqrt(2.0 / math.pi)

    def merge(b):
        for h in range(HEADS):
            inverse = 1.0 / acc[b, h, head:head + 1, :]
            blend[h * head:(h + 1) * head, :] = (acc[b, h, :head, :] * inverse).astype(BF16)

    def residual_jobs(b, r):
        part = block_rows // 2

        def job(k):
            at = slice(r * block_rows + k * part, r * block_rows + (k + 1) * part)
            to = slice(k * part, (k + 1) * part)
            middle = (own[b, at, :].astype(F32) + dot_tn(blend[:, at], wo[...])).astype(BF16)
            mid[2 * b + r, to, :] = middle
            second[2 * b + r, to, :] = normed(middle, gain2[...])

        return [functools.partial(job, k) for k in range(2)]

    def rise_jobs(b, r):
        def job(f):
            span = slice(f * wide, (f + 1) * wide)
            u = dot_nn(second[2 * b + r], wu[:, span])
            bent = jnp.tanh(u * (slope + (slope * 0.044715) * (u * u)))
            hid[2 * b + r, :, span] = (u + u * bent).astype(BF16)

        return [functools.partial(job, f) for f in range(inner // wide)]

    def fall_jobs(b, r):
        at = slice(r * block_rows, (r + 1) * block_rows)

        def job(span):
            down = dot_nn(hid[2 * b + r], wd[:, span])
            out_ref[b, at, span] = (mid[2 * b + r, :, span].astype(F32) + 0.5 * down).astype(BF16)

        return [functools.partial(job, span) for span in spans]

    def run(*queues):
        order = []
        for rank, queue in enumerate(queues):
            order += [((k + 0.5) / len(queue), rank, k) for k in range(len(queue))]
        for _, rank, k in sorted(order):
            queues[rank][k]()

    index = {}
    for p, entry in enumerate(pieces):
        index[(entry[0], entry[2])] = p

    def px(w, k):
        with jax.named_scope(f"px{w}{k}"):
            pass_x(index[(w, k)])

    def py(w, k):
        with jax.named_scope(f"py{w}{k}"):
            pass_y(index[(w, k)])

    def have(w):
        with jax.named_scope(f"have{w}"):
            arrive(w)

    def halo_ready(s):
        with jax.named_scope(f"halo{s}"):
            halo_wait(s)

    px(KEYS, 0)
    px(KEYS, 1)
    px(VALUES, 0)
    px(VALUES, 1)
    py(KEYS, 0)
    px(QUERIES, 0)
    py(KEYS, 1)
    px(QUERIES, 1)
    py(VALUES, 0)
    have(KEYS)
    with jax.named_scope("keys"):
        for b in range(members):
            run(key_jobs(xn.at[b], 1 + b, rows))
    py(VALUES, 1)
    px(OUTPUT, 0)
    py(QUERIES, 0)
    have(VALUES)
    py(QUERIES, 1)
    with jax.named_scope("values"):
        wv_t[...] = jnp.transpose(wv[...])
        for b in range(members):
            run(value_jobs(xn.at[b], 1 + b, rows))
    halo_ready(0)
    have(QUERIES)
    with jax.named_scope("queries"):
        wq_t[...] = jnp.transpose(wq[...])
        run(query_jobs(0), first_jobs)
    px(UP, 0)
    with jax.named_scope("own0"):
        run(own_jobs(0), query_jobs(1) + project_jobs(0))
    py(OUTPUT, 0)
    halo_ready(1)
    with jax.named_scope("own1"):
        run(own_jobs(1))
    px(UP, 1)
    with jax.named_scope("s0"):
        run(halo_jobs(0), project_jobs(1))
    halo_ready(2)
    px(DOWN, 0)
    with jax.named_scope("s1"):
        run(halo_jobs(1), project_jobs(2))
    py(UP, 0)
    halo_ready(3)
    with jax.named_scope("s2"):
        run(halo_jobs(2), project_jobs(3))
    px(DOWN, 1)
    halo_ready(4)
    with jax.named_scope("s3"):
        run(halo_jobs(3), project_jobs(4))
        merge(0)
    px(DOWN, 2)
    have(OUTPUT)
    with jax.named_scope("s4"):
        run(halo_jobs(4), residual_jobs(0, 0) + residual_jobs(0, 1))
    px(DOWN, 3)
    py(UP, 1)
    halo_ready(5)
    with jax.named_scope("s5"):
        run(project_jobs(5))
        run(halo_jobs(5))
    py(DOWN, 0)
    have(UP)
    with jax.named_scope("r00"):
        run(rise_jobs(0, 0))
    py(DOWN, 1)
    halo_ready(6)
    with jax.named_scope("s6"):
        run(project_jobs(6))
        run(halo_jobs(6), rise_jobs(0, 1)[:4])
    py(DOWN, 2)
    with jax.named_scope("r01"):
        run(rise_jobs(0, 1)[4:])
    halo_ready(7)
    py(DOWN, 3)
    with jax.named_scope("s7"):
        run(project_jobs(7))
        run(halo_jobs(7))
        merge(1)
        run(residual_jobs(1, 0))
    have(DOWN)
    with jax.named_scope("fin1"):
        run(rise_jobs(1, 0), residual_jobs(1, 1), fall_jobs(0, 0))
    with jax.named_scope("fin2"):
        run(rise_jobs(1, 1), fall_jobs(0, 1) + fall_jobs(1, 0))
        run(fall_jobs(1, 1))

    with jax.named_scope("sent"):
        remote(halo, halo, halo_send.at[0], halo_recv.at[0], (nxt, m)).wait_send()
        for w in range(n_weights):
            three = fulls[w].at[pl.ds(0, 3 * sources[w].shape[0]), :]
            remote(three, three, weight_send.at[w], mate_recv.at[w], mate).wait_send()


def solution(mesh):
    n_mesh, n_member = mesh.shape["mesh"], mesh.shape["member"]
    geometry = (n_mesh, 4, 2, n_member)

    def on_device(states, projection, output_w, up_w, down_w, gain1, gain2, lists, counts):
        members, rows, width = states.shape
        inner = up_w.shape[1]
        tiles = rows // TILE
        n_pieces = sum(n for _, n in SPLIT)
        hbm = pl.BlockSpec(memory_space=pl.ANY)
        vmem = pl.BlockSpec(memory_space=pltpu.VMEM)
        dma = pltpu.SemaphoreType.DMA
        return pl.pallas_call(
            functools.partial(layer_kernel, geometry),
            name="layer",
            out_shape=pltpu.VMEM(states.shape, BF16),
            in_specs=[hbm] * 9,
            out_specs=vmem,
            scratch_shapes=[
                pltpu.VMEM((members, rows, width), BF16),
                pltpu.VMEM((members, tiles, 2 * TILE, width), BF16),
                pltpu.VMEM((width, width), BF16),
                pltpu.VMEM((width, width), BF16),
                pltpu.VMEM((width, width), BF16),
                pltpu.VMEM((width, width), BF16),
                pltpu.VMEM((width, inner), BF16),
                pltpu.VMEM((inner, width), BF16),
                pltpu.VMEM((width, width), BF16),
                pltpu.VMEM((width, width), BF16),
                pltpu.VMEM((members, rows, width), BF16),
                pltpu.VMEM((2 * TILE, width), BF16),
                pltpu.VMEM((members, width, rows), BF16),
                pltpu.VMEM((3, HEADS, rows, width // HEADS), BF16),
                pltpu.VMEM((3, HEADS, width // HEADS + ONES, rows), BF16),
                pltpu.VMEM((members, HEADS, width // HEADS + ONES, rows), F32),
                pltpu.VMEM((members, HEADS, 1, rows), F32),
                pltpu.VMEM((tiles + 2 * RIM_T, rows), F32),
                pltpu.VMEM((HEADS, rows, rows), F32),
                pltpu.VMEM((4, rows // 2, inner), BF16),
                pltpu.VMEM((width, rows), BF16),
                pltpu.VMEM((4, rows // 2, width), BF16),
                pltpu.VMEM((4, rows // 2, width), BF16),
                pltpu.VMEM((1, width), F32), pltpu.VMEM((1, width), F32),
                pltpu.SMEM(lists.shape, jnp.int32), pltpu.SMEM(counts.shape, jnp.int32),
                dma((14,)),
                dma((1,)), dma((members * tiles,)),
                dma((6,)), dma((6,)), dma((n_pieces,)), dma((n_pieces,)),
            ],
            compiler_params=pltpu.CompilerParams(
                collective_id=0, has_side_effects=True, vmem_limit_bytes=60 * 1024 * 1024
            ),
        )(
            states, projection, output_w, up_w, down_w,
            gain1.reshape(1, width), gain2.reshape(1, width), lists, counts,
        )

    in_specs = (
        P("member", "mesh", None),
        P("member", None),
        P("member", None),
        P("member", None),
        P("member", None),
        P(),
        P(),
        P("mesh", None),
        P("mesh"),
    )
    return jax.shard_map(
        on_device, mesh=mesh, in_specs=in_specs, out_specs=P("member", "mesh", None), check_vma=False
    )
```

```python
import functools
import math

import jax
import jax.numpy as jnp
from jax import lax
from jax.experimental import pallas as pl
from jax.experimental.pallas import tpu as pltpu
from jax.sharding import PartitionSpec as P

HEADS = 4
TILE = 128
RIM_T = 4
HIDDEN_LOW = -1e30
ONES = 16
AHEAD = 4
MESH = pl.DeviceIdType.MESH
F32 = jnp.float32
BF16 = jnp.bfloat16

SPLIT = ((0, 2), (1, 2), (2, 2), (3, 1), (4, 2), (5, 4))
DIRECT = ((5, 3),)
KEYS, VALUES, QUERIES, OUTPUT, UP, DOWN = range(6)


def normed(values, gain):
    values = values.astype(F32)
    center = values - jnp.mean(values, axis=-1, keepdims=True)
    spread = jnp.mean(center * center, axis=-1, keepdims=True)
    return (center * lax.rsqrt(spread + 1e-05) * gain).astype(BF16)


def dot_nn(a, b):
    return jnp.dot(a, b, preferred_element_type=F32)


def dot_nt(a, b):
    return lax.dot_general(a, b, (((1,), (1,)), ((), ())), preferred_element_type=F32)


def dot_tn(a, b):
    return lax.dot_general(a, b, (((0,), (0,)), ((), ())), preferred_element_type=F32)


def layer_kernel(
    geometry,
    x_hbm, wp_hbm, wo_hbm, wu_hbm, wd_hbm, gain1_hbm, gain2_hbm, lists_hbm, counts_hbm,
    out_ref,
    own, halo, wk, wv, wq, wo, wu, wd, wq_t, wv_t, xn, hn, q_t, kc, v_t, acc, top, bias, scores, hid, blend,
    second, mid,
    gain1, gain2, lists, counts,
    loc_sem, halo_send, halo_recv, weight_send, mate_recv, x_recv, y_recv,
):
    n_mesh, n_z, n_x, n_member = geometry
    members, rows, width = x_hbm.shape
    tiles = rows // TILE
    head = width // HEADS
    i = lax.axis_index("mesh")
    m = lax.axis_index("member")
    nxt = (i + 1) % n_mesh
    prv = (i + n_mesh - 1) % n_mesh
    x_lo = (i // n_z) % n_x
    y = i // (n_z * n_x)
    half = y % 2
    plane = n_z * n_x
    cross = (i + n_z - 2 * n_z * x_lo, (m + 2) % n_member)
    mate = (i, m + 1 - 2 * (m % 2))
    y_to = ((i + n_mesh + plane * (2 * x_lo - 1)) % n_mesh, m)
    y_from = ((i + n_mesh - plane * (2 * x_lo - 1)) % n_mesh, m)
    far = (m + 2) % n_member
    mate_far = (mate[1] + 2) % n_member

    barrier = pltpu.get_barrier_semaphore()
    for peer in ((nxt, m), (prv, m), cross, mate, y_to, y_from):
        pl.semaphore_signal(barrier, inc=1, device_id=peer, device_id_type=MESH)

    sources = (
        wp_hbm.at[:, pl.ds(width, width)], wp_hbm.at[:, pl.ds(2 * width, width)], wp_hbm.at[:, pl.ds(0, width)],
        wo_hbm, wu_hbm, wd_hbm,
    )
    fulls = (wk, wv, wq, wo, wu, wd)
    n_weights = len(fulls)

    def shard(w, owner):
        r = sources[w].shape[0]
        return fulls[w].at[pl.ds(pl.multiple_of(owner * r, 16), r), :]

    def piece(w, n, k, owner, which):
        r = sources[w].shape[0]
        size = r // 2 // n
        start = owner * r + which * (r // 2) + k * size
        return fulls[w].at[pl.ds(pl.multiple_of(start, 16), size), :]

    loads = [pltpu.make_async_copy(sources[w], shard(w, m), loc_sem.at[w]) for w in range(n_weights)]
    spots = [(0, slice(0, TILE)), (0, slice(TILE, rows)), (1, slice(0, rows))]
    load_x = [
        pltpu.make_async_copy(x_hbm.at[b, at, :], own.at[b, at, :], loc_sem.at[n_weights + 5 + k])
        for k, (b, at) in enumerate(spots)
    ]
    smalls = [
        pltpu.make_async_copy(src, dst, loc_sem.at[n_weights + 1 + k])
        for k, (src, dst) in enumerate(
            ((lists_hbm, lists), (counts_hbm, counts), (gain1_hbm, gain1), (gain2_hbm, gain2))
        )
    ]
    for load in load_x[:1] + loads[:3] + load_x[1:] + loads[3:] + smalls:
        load.start()

    pieces = []
    for w, n in SPLIT:
        for k in range(n):
            pieces.append((w, n, k))

    def remote(src, dst, send, recv, peer):
        return pltpu.make_async_remote_copy(
            src_ref=src, dst_ref=dst, send_sem=send, recv_sem=recv, device_id=peer, device_id_type=MESH
        )

    def halo_copy(side, b, j):
        raw = b == 0 and j == 0
        src = (own if raw else xn).at[b, pl.ds(j * TILE, TILE), :]
        dst = halo.at[b, j, pl.ds(side * TILE, TILE), :]
        peer = (nxt, m) if side == 0 else (prv, m)
        return remote(src, dst, halo_send.at[0], halo_recv.at[tiles * b + j], peer)

    def mate_copy(w, owner):
        return remote(shard(w, owner), shard(w, owner), weight_send.at[w], mate_recv.at[w], mate)

    def x_copy(p, owner):
        ref = piece(*pieces[p], owner, half)
        return remote(ref, ref, weight_send.at[pieces[p][0]], x_recv.at[p], cross)

    def y_copy(p, which):
        ref = piece(*pieces[p], far, which)
        return remote(ref, ref, weight_send.at[pieces[p][0]], y_recv.at[p], y_to)

    def d_copy(p, which):
        ref = piece(*pieces[p], far, which)
        return remote(ref, ref, weight_send.at[pieces[p][0]], mate_recv.at[pieces[p][0]], mate)

    def straight(p):
        return (pieces[p][0], pieces[p][2]) in DIRECT

    def pass_x(p):
        x_copy(p, far).wait_recv()
        if not straight(p):
            y_copy(p, half).start()
        d_copy(p, half).start()

    def pass_y(p):
        y_copy(p, 1 - half).wait_recv()
        d_copy(p, 1 - half).start()

    def arrive(w):
        both = fulls[w].at[pl.ds(0, 2 * sources[w].shape[0]), :]
        remote(both, both, weight_send.at[w], mate_recv.at[w], mate).wait_recv()

    def send_weight(w):
        loads[w].wait()
        for p, entry in enumerate(pieces):
            if entry[0] == w:
                x_copy(p, m).start()
                if straight(p):
                    ref = piece(*entry, m, 1 - half)
                    remote(ref, ref, weight_send.at[w], y_recv.at[p], cross).start()
        mate_copy(w, m).start()

    with jax.named_scope("enter"):
        pl.semaphore_wait(barrier, 6)
    load_x[0].wait()
    for side in range(2):
        halo_copy(side, 0, 0).start()
    send_weight(KEYS)
    send_weight(VALUES)
    send_weight(QUERIES)
    load_x[1].wait()
    load_x[2].wait()
    def norm_own(k, _):
        b = k // tiles
        at = pl.ds(pl.multiple_of((k % tiles) * TILE, TILE), TILE)
        xn[b, at, :] = normed(own[b, at, :], gain1[...])
        return 0

    with jax.named_scope("norm_own"):
        smalls[2].wait()
        smalls[3].wait()
        for b in range(members):
            lax.fori_loop(b * tiles, (b + 1) * tiles, norm_own, 0)
            for j in range(tiles):
                if b + j > 0:
                    for side in range(2):
                        halo_copy(side, b, j).start()
        send_weight(OUTPUT)
        send_weight(UP)
        send_weight(DOWN)
    for small in smalls[:2]:
        small.wait()
    first = i * tiles - RIM_T
    all_tiles = n_mesh * tiles
    entries = lists.shape[1]
    locals_ = [[(lists[t, e] - first + all_tiles) % all_tiles for e in range(entries)] for t in range(tiles)]
    for kt in range(tiles + 2 * RIM_T):
        for t in range(tiles):
            hit = jnp.int32(0)
            for e in range(entries):
                used = jnp.logical_and(locals_[t][e] == kt, e < counts[t])
                hit = jnp.where(used, jnp.int32(1), hit)
            level = jnp.where(hit > 0, F32(0), F32(HIDDEN_LOW))
            bias[pl.ds(kt, 1), t * TILE:(t + 1) * TILE] = jnp.full((1, TILE), level, F32)


    steps = members * tiles

    def norm_first(k):
        part = slice(k * (TILE // 2), (k + 1) * (TILE // 2))
        hn[part, :] = normed(halo[0, 0, part, :], gain1[...])

    first_jobs = [functools.partial(norm_first, k) for k in range(4)]

    def halo_wait(s):
        chunk = halo.at[s // tiles, s % tiles]
        remote(chunk, chunk, halo_send.at[0], halo_recv.at[s], (nxt, m)).wait_recv()

    scale = F32(math.log2(math.e) / math.sqrt(head))

    for slot in range(3):
        for h in range(HEADS):
            v_t[slot, h, head:, :] = jnp.ones((ONES, rows), BF16)

    wide = 2 * TILE
    spans = [slice(c * wide, (c + 1) * wide) for c in range(width // wide)]

    def key_jobs(source, slot, n):
        def job(span):
            keys = dot_nn(source[...], wk[:, span]).astype(BF16)
            for k in range(wide // head):
                kc[slot, span.start // head + k, :n, :] = keys[:, k * head:(k + 1) * head]

        return [functools.partial(job, span) for span in spans]

    def value_jobs(source, slot, n):
        def job(span):
            values = dot_nt(wv_t[span, :], source[...]).astype(BF16)
            for k in range(wide // head):
                v_t[slot, span.start // head + k, :head, :n] = values[k * head:(k + 1) * head, :]

        return [functools.partial(job, span) for span in spans]

    def query_jobs(b):
        def job(span):
            q_t[b, span, :] = (dot_nt(wq_t[span, :], xn[b]) * scale).astype(BF16)

        return [functools.partial(job, span) for span in spans]

    def attend_jobs(b, slot, marks, opening):
        n = len(marks) * TILE
        blocks = [(h, cols) for h in range(HEADS) for cols in spans]

        def score(h, cols):
            feats = slice(h * head, (h + 1) * head)
            scores[h, :n, cols] = dot_nn(kc[slot, h, :n, :], q_t[b, feats, cols])

        def blend_in(h, cols):
            best = None if opening else top[b, h, :, cols]
            for k, mark in enumerate(marks):
                high = jnp.max(scores[h, k * TILE:(k + 1) * TILE, cols], axis=0, keepdims=True) + mark[:, cols]
                best = high if best is None else jnp.maximum(best, high)
            parts = [
                jnp.exp2(scores[h, k * TILE:(k + 1) * TILE, cols] - (best - mark[:, cols])).astype(BF16)
                for k, mark in enumerate(marks)
            ]
            product = dot_nn(v_t[slot, h, :, :n], jnp.concatenate(parts, axis=0))
            if opening:
                acc[b, h, :, cols] = product
            else:
                acc[b, h, :, cols] = acc[b, h, :, cols] * jnp.exp2(top[b, h, :, cols] - best) + product
            top[b, h, :, cols] = best

        def job(k):
            if k == 0:
                for block in blocks[:AHEAD]:
                    score(*block)
            if k + AHEAD < len(blocks):
                score(*blocks[k + AHEAD])
            blend_in(*blocks[k])

        return [functools.partial(job, k) for k in range(len(blocks))]

    def own_jobs(b):
        return attend_jobs(b, 1 + b, [bias[RIM_T + t:RIM_T + t + 1, :] for t in range(tiles)], True)

    def project_jobs(s):
        source, slot = hn if s == 0 else halo.at[s // tiles, s % tiles], s % 2
        return key_jobs(source, slot, 2 * TILE) + value_jobs(source, slot, 2 * TILE)

    def halo_jobs(s):
        b, j = s // tiles, s % tiles
        return attend_jobs(b, s % 2, [bias[j:j + 1, :], bias[j + RIM_T + tiles:j + RIM_T + tiles + 1, :]], False)

    block_rows = rows // 2
    inner = wu.shape[1]
    slope = math.sqrt(2.0 / math.pi)

    def merge(b):
        for h in range(HEADS):
            inverse = 1.0 / acc[b, h, head:head + 1, :]
            blend[h * head:(h + 1) * head, :] = (acc[b, h, :head, :] * inverse).astype(BF16)

    def residual_jobs(b, r):
        part = block_rows // 2

        def job(k):
            at = slice(r * block_rows + k * part, r * block_rows + (k + 1) * part)
            to = slice(k * part, (k + 1) * part)
            middle = (own[b, at, :].astype(F32) + dot_tn(blend[:, at], wo[...])).astype(BF16)
            mid[2 * b + r, to, :] = middle
            second[2 * b + r, to, :] = normed(middle, gain2[...])

        return [functools.partial(job, k) for k in range(2)]

    def rise_jobs(b, r):
        def job(f):
            span = slice(f * wide, (f + 1) * wide)
            u = dot_nn(second[2 * b + r], wu[:, span])
            bent = jnp.tanh(u * (slope + (slope * 0.044715) * (u * u)))
            hid[2 * b + r, :, span] = (u + u * bent).astype(BF16)

        return [functools.partial(job, f) for f in range(inner // wide)]

    def fall_jobs(b, r):
        at = slice(r * block_rows, (r + 1) * block_rows)

        def job(span):
            down = dot_nn(hid[2 * b + r], wd[:, span])
            out_ref[b, at, span] = (mid[2 * b + r, :, span].astype(F32) + 0.5 * down).astype(BF16)

        return [functools.partial(job, span) for span in spans]

    def run(*queues):
        order = []
        for rank, queue in enumerate(queues):
            order += [((k + 0.5) / len(queue), rank, k) for k in range(len(queue))]
        for _, rank, k in sorted(order):
            queues[rank][k]()

    index = {}
    for p, entry in enumerate(pieces):
        index[(entry[0], entry[2])] = p

    def px(w, k):
        with jax.named_scope(f"px{w}{k}"):
            pass_x(index[(w, k)])

    def py(w, k):
        with jax.named_scope(f"py{w}{k}"):
            pass_y(index[(w, k)])

    def have(w):
        with jax.named_scope(f"have{w}"):
            arrive(w)

    def halo_ready(s):
        with jax.named_scope(f"halo{s}"):
            halo_wait(s)

    px(KEYS, 0)
    px(KEYS, 1)
    px(VALUES, 0)
    px(VALUES, 1)
    py(KEYS, 0)
    px(QUERIES, 0)
    py(KEYS, 1)
    px(QUERIES, 1)
    py(VALUES, 0)
    have(KEYS)
    with jax.named_scope("keys"):
        for b in range(members):
            run(key_jobs(xn.at[b], 1 + b, rows))
    py(VALUES, 1)
    px(OUTPUT, 0)
    py(QUERIES, 0)
    py(QUERIES, 1)
    have(VALUES)
    with jax.named_scope("values"):
        wv_t[...] = jnp.transpose(wv[...])
        for b in range(members):
            run(value_jobs(xn.at[b], 1 + b, rows))
    halo_ready(0)
    have(QUERIES)
    with jax.named_scope("queries"):
        wq_t[...] = jnp.transpose(wq[...])
        run(query_jobs(0), first_jobs)
    px(UP, 0)
    with jax.named_scope("own0"):
        run(own_jobs(0), query_jobs(1) + project_jobs(0))
    py(OUTPUT, 0)
    halo_ready(1)
    with jax.named_scope("own1"):
        run(own_jobs(1))
    px(UP, 1)
    with jax.named_scope("s0"):
        run(halo_jobs(0), project_jobs(1))
    halo_ready(2)
    px(DOWN, 0)
    with jax.named_scope("s1"):
        run(halo_jobs(1), project_jobs(2))
    py(UP, 0)
    halo_ready(3)
    with jax.named_scope("s2"):
        run(halo_jobs(2), project_jobs(3))
    px(DOWN, 1)
    halo_ready(4)
    with jax.named_scope("s3"):
        run(halo_jobs(3), project_jobs(4))
        merge(0)
    px(DOWN, 2)
    have(OUTPUT)
    with jax.named_scope("s4"):
        run(halo_jobs(4), residual_jobs(0, 0) + residual_jobs(0, 1))
    px(DOWN, 3)
    py(UP, 1)
    halo_ready(5)
    with jax.named_scope("s5"):
        run(project_jobs(5))
        run(halo_jobs(5))
    py(DOWN, 0)
    have(UP)
    with jax.named_scope("r00"):
        run(rise_jobs(0, 0))
    py(DOWN, 1)
    halo_ready(6)
    with jax.named_scope("s6"):
        run(project_jobs(6))
        run(halo_jobs(6), rise_jobs(0, 1)[:4])
    py(DOWN, 3)
    py(DOWN, 2)
    with jax.named_scope("r01"):
        run(rise_jobs(0, 1)[4:])
    halo_ready(7)
    with jax.named_scope("s7a"):
        run(project_jobs(7))
    with jax.named_scope("s7b"):
        run(halo_jobs(7))
        merge(1)
        run(residual_jobs(1, 0))
    have(DOWN)
    with jax.named_scope("fin1"):
        run(rise_jobs(1, 0), residual_jobs(1, 1), fall_jobs(0, 0))
    with jax.named_scope("fin2"):
        run(rise_jobs(1, 1), fall_jobs(0, 1) + fall_jobs(1, 0))
        run(fall_jobs(1, 1))

    with jax.named_scope("sent"):
        remote(halo, halo, halo_send.at[0], halo_recv.at[0], (nxt, m)).wait_send()
        for w in range(n_weights):
            three = fulls[w].at[pl.ds(0, 3 * sources[w].shape[0]), :]
            remote(three, three, weight_send.at[w], mate_recv.at[w], mate).wait_send()


def solution(mesh):
    n_mesh, n_member = mesh.shape["mesh"], mesh.shape["member"]
    geometry = (n_mesh, 4, 2, n_member)

    def on_device(states, projection, output_w, up_w, down_w, gain1, gain2, lists, counts):
        members, rows, width = states.shape
        inner = up_w.shape[1]
        tiles = rows // TILE
        n_pieces = sum(n for _, n in SPLIT)
        hbm = pl.BlockSpec(memory_space=pl.ANY)
        vmem = pl.BlockSpec(memory_space=pltpu.VMEM)
        dma = pltpu.SemaphoreType.DMA
        return pl.pallas_call(
            functools.partial(layer_kernel, geometry),
            name="layer",
            out_shape=pltpu.VMEM(states.shape, BF16),
            in_specs=[hbm] * 9,
            out_specs=vmem,
            scratch_shapes=[
                pltpu.VMEM((members, rows, width), BF16),
                pltpu.VMEM((members, tiles, 2 * TILE, width), BF16),
                pltpu.VMEM((width, width), BF16),
                pltpu.VMEM((width, width), BF16),
                pltpu.VMEM((width, width), BF16),
                pltpu.VMEM((width, width), BF16),
                pltpu.VMEM((width, inner), BF16),
                pltpu.VMEM((inner, width), BF16),
                pltpu.VMEM((width, width), BF16),
                pltpu.VMEM((width, width), BF16),
                pltpu.VMEM((members, rows, width), BF16),
                pltpu.VMEM((2 * TILE, width), BF16),
                pltpu.VMEM((members, width, rows), BF16),
                pltpu.VMEM((3, HEADS, rows, width // HEADS), BF16),
                pltpu.VMEM((3, HEADS, width // HEADS + ONES, rows), BF16),
                pltpu.VMEM((members, HEADS, width // HEADS + ONES, rows), F32),
                pltpu.VMEM((members, HEADS, 1, rows), F32),
                pltpu.VMEM((tiles + 2 * RIM_T, rows), F32),
                pltpu.VMEM((HEADS, rows, rows), F32),
                pltpu.VMEM((4, rows // 2, inner), BF16),
                pltpu.VMEM((width, rows), BF16),
                pltpu.VMEM((4, rows // 2, width), BF16),
                pltpu.VMEM((4, rows // 2, width), BF16),
                pltpu.VMEM((1, width), F32), pltpu.VMEM((1, width), F32),
                pltpu.SMEM(lists.shape, jnp.int32), pltpu.SMEM(counts.shape, jnp.int32),
                dma((14,)),
                dma((1,)), dma((members * tiles,)),
                dma((6,)), dma((6,)), dma((n_pieces,)), dma((n_pieces,)),
            ],
            compiler_params=pltpu.CompilerParams(
                collective_id=0, has_side_effects=True, vmem_limit_bytes=60 * 1024 * 1024
            ),
        )(
            states, projection, output_w, up_w, down_w,
            gain1.reshape(1, width), gain2.reshape(1, width), lists, counts,
        )

    in_specs = (
        P("member", "mesh", None),
        P("member", None),
        P("member", None),
        P("member", None),
        P("member", None),
        P(),
        P(),
        P("mesh", None),
        P("mesh"),
    )
    return jax.shard_map(
        on_device, mesh=mesh, in_specs=in_specs, out_specs=P("member", "mesh", None), check_vma=False
    )
```

```python
import functools
import math

import jax
import jax.numpy as jnp
from jax import lax
from jax.experimental import pallas as pl
from jax.experimental.pallas import tpu as pltpu
from jax.sharding import PartitionSpec as P

HEADS = 4
TILE = 128
RIM_T = 4
HIDDEN_LOW = -1e30
ONES = 16
AHEAD = 6
MESH = pl.DeviceIdType.MESH
F32 = jnp.float32
BF16 = jnp.bfloat16

SPLIT = ((0, 2), (1, 2), (2, 2), (3, 1), (4, 2), (5, 4))
DIRECT = ((5, 3),)
KEYS, VALUES, QUERIES, OUTPUT, UP, DOWN = range(6)


def normed(values, gain):
    values = values.astype(F32)
    center = values - jnp.mean(values, axis=-1, keepdims=True)
    spread = jnp.mean(center * center, axis=-1, keepdims=True)
    return (center * lax.rsqrt(spread + 1e-05) * gain).astype(BF16)


def dot_nn(a, b):
    return jnp.dot(a, b, preferred_element_type=F32)


def dot_nt(a, b):
    return lax.dot_general(a, b, (((1,), (1,)), ((), ())), preferred_element_type=F32)


def dot_tn(a, b):
    return lax.dot_general(a, b, (((0,), (0,)), ((), ())), preferred_element_type=F32)


def layer_kernel(
    geometry,
    x_hbm, wp_hbm, wo_hbm, wu_hbm, wd_hbm, gain1_hbm, gain2_hbm, lists_hbm, counts_hbm,
    out_ref,
    own, halo, wk, wv, wq, wo, wu, wd, wq_t, wv_t, xn, hn, q_t, kc, v_t, acc, top, bias, scores, hid, blend,
    second, mid,
    gain1, gain2, lists, counts,
    loc_sem, halo_send, halo_recv, weight_send, mate_recv, x_recv, y_recv,
):
    n_mesh, n_z, n_x, n_member = geometry
    members, rows, width = x_hbm.shape
    tiles = rows // TILE
    head = width // HEADS
    i = lax.axis_index("mesh")
    m = lax.axis_index("member")
    nxt = (i + 1) % n_mesh
    prv = (i + n_mesh - 1) % n_mesh
    x_lo = (i // n_z) % n_x
    y = i // (n_z * n_x)
    half = y % 2
    plane = n_z * n_x
    cross = (i + n_z - 2 * n_z * x_lo, (m + 2) % n_member)
    mate = (i, m + 1 - 2 * (m % 2))
    y_to = ((i + n_mesh + plane * (2 * x_lo - 1)) % n_mesh, m)
    y_from = ((i + n_mesh - plane * (2 * x_lo - 1)) % n_mesh, m)
    far = (m + 2) % n_member
    mate_far = (mate[1] + 2) % n_member

    barrier = pltpu.get_barrier_semaphore()
    for peer in ((nxt, m), (prv, m), cross, mate, y_to, y_from):
        pl.semaphore_signal(barrier, inc=1, device_id=peer, device_id_type=MESH)

    sources = (
        wp_hbm.at[:, pl.ds(width, width)], wp_hbm.at[:, pl.ds(2 * width, width)], wp_hbm.at[:, pl.ds(0, width)],
        wo_hbm, wu_hbm, wd_hbm,
    )
    fulls = (wk, wv, wq, wo, wu, wd)
    n_weights = len(fulls)

    def shard(w, owner):
        r = sources[w].shape[0]
        return fulls[w].at[pl.ds(pl.multiple_of(owner * r, 16), r), :]

    def piece(w, n, k, owner, which):
        r = sources[w].shape[0]
        size = r // 2 // n
        start = owner * r + which * (r // 2) + k * size
        return fulls[w].at[pl.ds(pl.multiple_of(start, 16), size), :]

    loads = [pltpu.make_async_copy(sources[w], shard(w, m), loc_sem.at[w]) for w in range(n_weights)]
    spots = [(0, slice(0, TILE)), (0, slice(TILE, rows)), (1, slice(0, rows))]
    load_x = [
        pltpu.make_async_copy(x_hbm.at[b, at, :], own.at[b, at, :], loc_sem.at[n_weights + 5 + k])
        for k, (b, at) in enumerate(spots)
    ]
    smalls = [
        pltpu.make_async_copy(src, dst, loc_sem.at[n_weights + 1 + k])
        for k, (src, dst) in enumerate(
            ((lists_hbm, lists), (counts_hbm, counts), (gain1_hbm, gain1), (gain2_hbm, gain2))
        )
    ]
    for load in load_x[:1] + loads[:3] + load_x[1:] + loads[3:] + smalls:
        load.start()

    pieces = []
    for w, n in SPLIT:
        for k in range(n):
            pieces.append((w, n, k))

    def remote(src, dst, send, recv, peer):
        return pltpu.make_async_remote_copy(
            src_ref=src, dst_ref=dst, send_sem=send, recv_sem=recv, device_id=peer, device_id_type=MESH
        )

    def halo_copy(side, b, j):
        raw = b == 0 and j == 0
        src = (own if raw else xn).at[b, pl.ds(j * TILE, TILE), :]
        dst = halo.at[b, j, pl.ds(side * TILE, TILE), :]
        peer = (nxt, m) if side == 0 else (prv, m)
        return remote(src, dst, halo_send.at[0], halo_recv.at[tiles * b + j], peer)

    def mate_copy(w, owner):
        return remote(shard(w, owner), shard(w, owner), weight_send.at[w], mate_recv.at[w], mate)

    def x_copy(p, owner):
        ref = piece(*pieces[p], owner, half)
        return remote(ref, ref, weight_send.at[pieces[p][0]], x_recv.at[p], cross)

    def y_copy(p, which):
        ref = piece(*pieces[p], far, which)
        return remote(ref, ref, weight_send.at[pieces[p][0]], y_recv.at[p], y_to)

    def d_copy(p, which):
        ref = piece(*pieces[p], far, which)
        return remote(ref, ref, weight_send.at[pieces[p][0]], mate_recv.at[pieces[p][0]], mate)

    def straight(p):
        return (pieces[p][0], pieces[p][2]) in DIRECT

    def pass_x(p):
        x_copy(p, far).wait_recv()
        if not straight(p):
            y_copy(p, half).start()
        d_copy(p, half).start()

    def pass_y(p):
        y_copy(p, 1 - half).wait_recv()
        d_copy(p, 1 - half).start()

    def arrive(w):
        both = fulls[w].at[pl.ds(0, 2 * sources[w].shape[0]), :]
        remote(both, both, weight_send.at[w], mate_recv.at[w], mate).wait_recv()

    def send_weight(w):
        loads[w].wait()
        for p, entry in enumerate(pieces):
            if entry[0] == w:
                x_copy(p, m).start()
                if straight(p):
                    ref = piece(*entry, m, 1 - half)
                    remote(ref, ref, weight_send.at[w], y_recv.at[p], cross).start()
        mate_copy(w, m).start()

    with jax.named_scope("enter"):
        pl.semaphore_wait(barrier, 6)
    load_x[0].wait()
    for side in range(2):
        halo_copy(side, 0, 0).start()
    send_weight(KEYS)
    send_weight(VALUES)
    send_weight(QUERIES)
    load_x[1].wait()
    load_x[2].wait()
    def norm_own(k, _):
        b = k // tiles
        at = pl.ds(pl.multiple_of((k % tiles) * TILE, TILE), TILE)
        xn[b, at, :] = normed(own[b, at, :], gain1[...])
        return 0

    with jax.named_scope("norm_own"):
        smalls[2].wait()
        smalls[3].wait()
        for b in range(members):
            lax.fori_loop(b * tiles, (b + 1) * tiles, norm_own, 0)
            for j in range(tiles):
                if b + j > 0:
                    for side in range(2):
                        halo_copy(side, b, j).start()
        send_weight(OUTPUT)
        send_weight(UP)
        send_weight(DOWN)
    for small in smalls[:2]:
        small.wait()
    first = i * tiles - RIM_T
    all_tiles = n_mesh * tiles
    entries = lists.shape[1]
    locals_ = [[(lists[t, e] - first + all_tiles) % all_tiles for e in range(entries)] for t in range(tiles)]
    for kt in range(tiles + 2 * RIM_T):
        for t in range(tiles):
            hit = jnp.int32(0)
            for e in range(entries):
                used = jnp.logical_and(locals_[t][e] == kt, e < counts[t])
                hit = jnp.where(used, jnp.int32(1), hit)
            level = jnp.where(hit > 0, F32(0), F32(HIDDEN_LOW))
            bias[pl.ds(kt, 1), t * TILE:(t + 1) * TILE] = jnp.full((1, TILE), level, F32)


    steps = members * tiles

    def norm_first(k):
        part = slice(k * (TILE // 2), (k + 1) * (TILE // 2))
        hn[part, :] = normed(halo[0, 0, part, :], gain1[...])

    first_jobs = [functools.partial(norm_first, k) for k in range(4)]

    def halo_wait(s):
        chunk = halo.at[s // tiles, s % tiles]
        remote(chunk, chunk, halo_send.at[0], halo_recv.at[s], (nxt, m)).wait_recv()

    scale = F32(math.log2(math.e) / math.sqrt(head))

    for slot in range(3):
        for h in range(HEADS):
            v_t[slot, h, head:, :] = jnp.ones((ONES, rows), BF16)

    wide = 2 * TILE
    spans = [slice(c * wide, (c + 1) * wide) for c in range(width // wide)]

    def key_jobs(source, slot, n):
        def job(span):
            keys = dot_nn(source[...], wk[:, span]).astype(BF16)
            for k in range(wide // head):
                kc[slot, span.start // head + k, :n, :] = keys[:, k * head:(k + 1) * head]

        return [functools.partial(job, span) for span in spans]

    def value_jobs(source, slot, n):
        def job(span):
            values = dot_nt(wv_t[span, :], source[...]).astype(BF16)
            for k in range(wide // head):
                v_t[slot, span.start // head + k, :head, :n] = values[k * head:(k + 1) * head, :]

        return [functools.partial(job, span) for span in spans]

    def query_jobs(b):
        def job(span):
            q_t[b, span, :] = (dot_nt(wq_t[span, :], xn[b]) * scale).astype(BF16)

        return [functools.partial(job, span) for span in spans]

    def attend_jobs(b, slot, marks, opening):
        n = len(marks) * TILE
        blocks = [(h, cols) for h in range(HEADS) for cols in spans]

        def score(h, cols):
            feats = slice(h * head, (h + 1) * head)
            scores[h, :n, cols] = dot_nn(kc[slot, h, :n, :], q_t[b, feats, cols])

        def blend_in(h, cols):
            best = None if opening else top[b, h, :, cols]
            for k, mark in enumerate(marks):
                high = jnp.max(scores[h, k * TILE:(k + 1) * TILE, cols], axis=0, keepdims=True) + mark[:, cols]
                best = high if best is None else jnp.maximum(best, high)
            parts = [
                jnp.exp2(scores[h, k * TILE:(k + 1) * TILE, cols] - (best - mark[:, cols])).astype(BF16)
                for k, mark in enumerate(marks)
            ]
            product = dot_nn(v_t[slot, h, :, :n], jnp.concatenate(parts, axis=0))
            if opening:
                acc[b, h, :, cols] = product
            else:
                acc[b, h, :, cols] = acc[b, h, :, cols] * jnp.exp2(top[b, h, :, cols] - best) + product
            top[b, h, :, cols] = best

        def job(k):
            if k == 0:
                for block in blocks[:AHEAD]:
                    score(*block)
            if k + AHEAD < len(blocks):
                score(*blocks[k + AHEAD])
            blend_in(*blocks[k])

        return [functools.partial(job, k) for k in range(len(blocks))]

    def own_jobs(b):
        return attend_jobs(b, 1 + b, [bias[RIM_T + t:RIM_T + t + 1, :] for t in range(tiles)], True)

    def project_jobs(s):
        source, slot = hn if s == 0 else halo.at[s // tiles, s % tiles], s % 2
        return key_jobs(source, slot, 2 * TILE) + value_jobs(source, slot, 2 * TILE)

    def halo_jobs(s):
        b, j = s // tiles, s % tiles
        return attend_jobs(b, s % 2, [bias[j:j + 1, :], bias[j + RIM_T + tiles:j + RIM_T + tiles + 1, :]], False)

    block_rows = rows // 2
    inner = wu.shape[1]
    slope = math.sqrt(2.0 / math.pi)

    def merge(b):
        for h in range(HEADS):
            inverse = 1.0 / acc[b, h, head:head + 1, :]
            blend[h * head:(h + 1) * head, :] = (acc[b, h, :head, :] * inverse).astype(BF16)

    def residual_jobs(b, r):
        part = block_rows // 2

        def job(k):
            at = slice(r * block_rows + k * part, r * block_rows + (k + 1) * part)
            to = slice(k * part, (k + 1) * part)
            middle = (own[b, at, :].astype(F32) + dot_tn(blend[:, at], wo[...])).astype(BF16)
            mid[2 * b + r, to, :] = middle
            second[2 * b + r, to, :] = normed(middle, gain2[...])

        return [functools.partial(job, k) for k in range(2)]

    def rise_jobs(b, r):
        def job(f):
            span = slice(f * wide, (f + 1) * wide)
            u = dot_nn(second[2 * b + r], wu[:, span])
            bent = jnp.tanh(u * (slope + (slope * 0.044715) * (u * u)))
            hid[2 * b + r, :, span] = (u + u * bent).astype(BF16)

        return [functools.partial(job, f) for f in range(inner // wide)]

    def fall_jobs(b, r):
        at = slice(r * block_rows, (r + 1) * block_rows)

        def job(span):
            down = dot_nn(hid[2 * b + r], wd[:, span])
            out_ref[b, at, span] = (mid[2 * b + r, :, span].astype(F32) + 0.5 * down).astype(BF16)

        return [functools.partial(job, span) for span in spans]

    def run(*queues):
        order = []
        for rank, queue in enumerate(queues):
            order += [((k + 0.5) / len(queue), rank, k) for k in range(len(queue))]
        for _, rank, k in sorted(order):
            queues[rank][k]()

    index = {}
    for p, entry in enumerate(pieces):
        index[(entry[0], entry[2])] = p

    def px(w, k):
        with jax.named_scope(f"px{w}{k}"):
            pass_x(index[(w, k)])

    def py(w, k):
        with jax.named_scope(f"py{w}{k}"):
            pass_y(index[(w, k)])

    def have(w):
        with jax.named_scope(f"have{w}"):
            arrive(w)

    def halo_ready(s):
        with jax.named_scope(f"halo{s}"):
            halo_wait(s)

    px(KEYS, 0)
    px(KEYS, 1)
    px(VALUES, 0)
    px(VALUES, 1)
    py(KEYS, 0)
    px(QUERIES, 0)
    py(KEYS, 1)
    px(QUERIES, 1)
    py(VALUES, 0)
    have(KEYS)
    with jax.named_scope("keys"):
        for b in range(members):
            run(key_jobs(xn.at[b], 1 + b, rows))
    py(VALUES, 1)
    px(OUTPUT, 0)
    py(QUERIES, 0)
    py(QUERIES, 1)
    have(VALUES)
    with jax.named_scope("values"):
        wv_t[...] = jnp.transpose(wv[...])
        for b in range(members):
            run(value_jobs(xn.at[b], 1 + b, rows))
    halo_ready(0)
    have(QUERIES)
    with jax.named_scope("queries"):
        wq_t[...] = jnp.transpose(wq[...])
        run(query_jobs(0), first_jobs)
    px(UP, 0)
    with jax.named_scope("own0"):
        run(own_jobs(0), query_jobs(1) + project_jobs(0))
    py(OUTPUT, 0)
    halo_ready(1)
    with jax.named_scope("own1"):
        run(own_jobs(1))
    px(UP, 1)
    with jax.named_scope("s0"):
        run(halo_jobs(0), project_jobs(1))
    halo_ready(2)
    px(DOWN, 0)
    with jax.named_scope("s1"):
        run(halo_jobs(1), project_jobs(2))
    py(UP, 0)
    halo_ready(3)
    with jax.named_scope("s2"):
        run(halo_jobs(2), project_jobs(3))
    px(DOWN, 1)
    halo_ready(4)
    with jax.named_scope("s3"):
        run(halo_jobs(3), project_jobs(4))
        merge(0)
    px(DOWN, 2)
    have(OUTPUT)
    with jax.named_scope("s4"):
        run(halo_jobs(4), residual_jobs(0, 0) + residual_jobs(0, 1))
    px(DOWN, 3)
    py(UP, 1)
    halo_ready(5)
    with jax.named_scope("s5"):
        run(project_jobs(5))
        run(halo_jobs(5))
    py(DOWN, 0)
    have(UP)
    with jax.named_scope("r00"):
        run(rise_jobs(0, 0))
    py(DOWN, 1)
    halo_ready(6)
    with jax.named_scope("s6"):
        run(project_jobs(6))
        run(halo_jobs(6), rise_jobs(0, 1)[:4])
    py(DOWN, 3)
    py(DOWN, 2)
    with jax.named_scope("r01"):
        run(rise_jobs(0, 1)[4:])
    halo_ready(7)
    with jax.named_scope("s7a"):
        run(project_jobs(7))
    with jax.named_scope("s7b"):
        run(halo_jobs(7))
        merge(1)
        run(residual_jobs(1, 0))
    have(DOWN)
    with jax.named_scope("fin1"):
        run(rise_jobs(1, 0), residual_jobs(1, 1), fall_jobs(0, 0) + fall_jobs(0, 1))
    with jax.named_scope("fin2"):
        run(rise_jobs(1, 1), fall_jobs(1, 0))
        run(fall_jobs(1, 1))

    with jax.named_scope("sent"):
        remote(halo, halo, halo_send.at[0], halo_recv.at[0], (nxt, m)).wait_send()
        for w in range(n_weights):
            three = fulls[w].at[pl.ds(0, 3 * sources[w].shape[0]), :]
            remote(three, three, weight_send.at[w], mate_recv.at[w], mate).wait_send()


def solution(mesh):
    n_mesh, n_member = mesh.shape["mesh"], mesh.shape["member"]
    geometry = (n_mesh, 4, 2, n_member)

    def on_device(states, projection, output_w, up_w, down_w, gain1, gain2, lists, counts):
        members, rows, width = states.shape
        inner = up_w.shape[1]
        tiles = rows // TILE
        n_pieces = sum(n for _, n in SPLIT)
        hbm = pl.BlockSpec(memory_space=pl.ANY)
        vmem = pl.BlockSpec(memory_space=pltpu.VMEM)
        dma = pltpu.SemaphoreType.DMA
        return pl.pallas_call(
            functools.partial(layer_kernel, geometry),
            name="layer",
            out_shape=pltpu.VMEM(states.shape, BF16),
            in_specs=[hbm] * 9,
            out_specs=vmem,
            scratch_shapes=[
                pltpu.VMEM((members, rows, width), BF16),
                pltpu.VMEM((members, tiles, 2 * TILE, width), BF16),
                pltpu.VMEM((width, width), BF16),
                pltpu.VMEM((width, width), BF16),
                pltpu.VMEM((width, width), BF16),
                pltpu.VMEM((width, width), BF16),
                pltpu.VMEM((width, inner), BF16),
                pltpu.VMEM((inner, width), BF16),
                pltpu.VMEM((width, width), BF16),
                pltpu.VMEM((width, width), BF16),
                pltpu.VMEM((members, rows, width), BF16),
                pltpu.VMEM((2 * TILE, width), BF16),
                pltpu.VMEM((members, width, rows), BF16),
                pltpu.VMEM((3, HEADS, rows, width // HEADS), BF16),
                pltpu.VMEM((3, HEADS, width // HEADS + ONES, rows), BF16),
                pltpu.VMEM((members, HEADS, width // HEADS + ONES, rows), F32),
                pltpu.VMEM((members, HEADS, 1, rows), F32),
                pltpu.VMEM((tiles + 2 * RIM_T, rows), F32),
                pltpu.VMEM((HEADS, rows, rows), F32),
                pltpu.VMEM((4, rows // 2, inner), BF16),
                pltpu.VMEM((width, rows), BF16),
                pltpu.VMEM((4, rows // 2, width), BF16),
                pltpu.VMEM((4, rows // 2, width), BF16),
                pltpu.VMEM((1, width), F32), pltpu.VMEM((1, width), F32),
                pltpu.SMEM(lists.shape, jnp.int32), pltpu.SMEM(counts.shape, jnp.int32),
                dma((14,)),
                dma((1,)), dma((members * tiles,)),
                dma((6,)), dma((6,)), dma((n_pieces,)), dma((n_pieces,)),
            ],
            compiler_params=pltpu.CompilerParams(
                collective_id=0, has_side_effects=True, vmem_limit_bytes=60 * 1024 * 1024
            ),
        )(
            states, projection, output_w, up_w, down_w,
            gain1.reshape(1, width), gain2.reshape(1, width), lists, counts,
        )

    in_specs = (
        P("member", "mesh", None),
        P("member", None),
        P("member", None),
        P("member", None),
        P("member", None),
        P(),
        P(),
        P("mesh", None),
        P("mesh"),
    )
    return jax.shard_map(
        on_device, mesh=mesh, in_specs=in_specs, out_specs=P("member", "mesh", None), check_vma=False
    )
```
